32 devices in a mesh: groups: 2 (over y), bank: 4 (over z), freq: 2 (over x), seg: 2 (over core).
Axes of the slice: x: 2, y: 2, z: 4, core: 2. Of those that a mesh axis runs over, the one named last changes fastest.
Arguments:
- coarse_spectra: bfloat16 [64, 2, 16384], P(('groups', 'seg', 'bank'), None, 'freq'), parts along dimension 0, may hold values from -6 to 6
- fine_spectra: bfloat16 [64, 2, 65536], P(('groups', 'seg', 'bank'), None, 'freq'), parts along dimension 0, may hold values from -6 to 6
- coarse_templates: bfloat16 [2, 2048, 16384], P(None, 'bank', 'freq'), may hold values from -6 to 6
- fine_templates: bfloat16 [2, 4, 64, 65536], P(None, 'bank', None, 'freq'), may hold values from -6 to 6
- coarse_weight: float32 [32768], P(('groups', 'freq')), parts along dimension 0, may hold values from 0.2 to 2
- fine_weight: float32 [131072], P(('groups', 'freq')), parts along dimension 0, may hold values from 0.2 to 2
- triggers: int32 [64, 2], P(('groups', 'seg')), parts along dimension 0, may hold values from 0 to 3, all different within a row; in each aligned block of 4 rows (0 to 3, 4 to 7, ...) at most 2 rows name the same one
- offsets: int32 [64, 2], P(('groups', 'seg')), parts along dimension 0, may hold values from 0 to 131056
Outputs:
- coarse_snr: float32 [2048, 64], P(('bank', 'freq'), ('groups', 'seg')), parts along dimension 1
- fine_snr: float32 [64, 2, 64], P(('groups', 'seg', 'bank'), None, 'freq'), parts along dimension 0
The draws below stay inside these ranges and needn't reach their ends.
There are 2 independent parts, one for each index of `groups`. The reference program is written for one: setup_inputs(seed, part) draws one part's arguments, and reference() takes and returns one part's arrays. A program takes and returns all parts, laid end to end along the dimension named above; an argument that names none is the same for every part. Nothing has to cross between parts.
Inputs may be any that keep to these rules, and one draw needn't show every extreme that they name: `triggers`: each segment names 2 different sub-banks. In each aligned block of 4 segments (the segments of one device along seg and bank) no sub-bank is named more than 2 times.
All inputs are finite; a program needn't handle non-finite values.
Results may differ from the reference program's by a relative error of at most 0.0021.
Values may be sent and summed in bfloat16 or wider, within the bound.
No kernel may reach another device: no remote copies, remote signals or barrier semaphores. Data moves between devices by JAX's collectives and lax.ppermute only.
A program may use at most 128 MiB of HBM per device.

```python
import math
import jax
import jax.numpy as jnp
import numpy as np
from jax import lax

FC = 16384
FB = 65536
TC = 2048
TSUB = 64
SEG_DEV = 4
TOP = 2
CAP = 2
LC = 16
LF = 16
CSTRIDE = 2047
SUBBANKS = 4
SEGS = 32


def place_ends(values, rng, smallest, largest):
    spot = [jax.random.randint(jax.random.fold_in(rng, axis), (), 0, length) for axis, length in enumerate(values.shape)]
    main_axis = values.shape.index(max(values.shape))
    beside = spot[:main_axis] + [(spot[main_axis] + 1) % values.shape[main_axis]] + spot[main_axis + 1:]
    return values.at[tuple(spot)].set(smallest).at[tuple(beside)].set(largest)


def block_levels(stream_key, dims, shards, smallest, largest):
    loudness, own = 1.0, jax.random.fold_in(stream_key, 6)
    for position, parts in shards:
        steps = jnp.exp(jax.random.uniform(jax.random.fold_in(own, position), (parts,), jnp.float32, smallest / len(shards), largest / len(shards)))
        loudness = loudness * jnp.repeat(steps, dims[position] // parts).reshape([-1 if axis == position else 1 for axis in range(len(dims))])
    return loudness


def shared_out(stream_key, own, number, rows, count, top, reach, skew):
    ranking = jax.random.permutation(stream_key, count)
    packed, ordinary = portions_of(count, rows * top, reach, skew, True), portions_of(count, rows * top, reach, skew, False)
    places = jnp.arange(count)

    def named(lengths, rotation):
        used = int((lengths > 0).sum())
        fixed = max(1, used // 4)
        passed = fixed + (places - fixed + rotation * (used - fixed)) % max(1, count - fixed)
        return jnp.zeros((count,), jnp.int32).at[ranking[jnp.where(places < fixed, places, passed)]].set(jnp.asarray(lengths, jnp.int32))

    lengths = jnp.where(number % 4 == 0, named(packed, number // 4), named(ordinary, number - number // 4 - 1))
    mixed = jax.random.permutation(jax.random.fold_in(own, 3), count)
    source_of, sink = mixed[0:count // 2 * 2:2], mixed[1:count // 2 * 2:2]
    margin = jnp.minimum(lengths[source_of] - 1, reach - lengths[sink]) // 2
    margin = jnp.where((source_of == ranking[0]) | (sink == ranking[0]) | (lengths[sink] == 0), 0, jnp.maximum(margin, 0))
    passed = jax.random.randint(jax.random.fold_in(own, 4), (count // 2,), 0, 1 << 20) % (margin + 1)
    lengths = lengths.at[source_of].add(-passed).at[sink].add(passed)
    labels = jnp.searchsorted(jnp.cumsum(lengths), jnp.arange(rows * top), side="right").astype(jnp.int32)
    table = labels.reshape(top, rows).T
    table = table[jax.random.permutation(jax.random.fold_in(own, 1), rows)]
    rotation = jax.random.randint(jax.random.fold_in(own, 2), (rows, 1), 0, top)
    return jnp.take_along_axis(table, (jnp.arange(top)[None, :] + rotation) % top, axis=1)


def portions_of(amount, total, bound, skew, full):
    portions = [(1 << 20) // math.isqrt(standing ** skew) + 1 for standing in range(1, amount + 1)]
    largest = bound if full else min(bound, max(-(-total // amount), total * portions[0] // sum(portions)))
    least = 1 if total - largest >= amount - 1 else 0
    given, rest = [largest] + [least] * (amount - 1), total - largest - least * (amount - 1)
    while rest > 0:
        free = [i for i in range(1, amount) if given[i] < largest] or [i for i in range(1, amount) if given[i] < bound]
        pool, left = sum([portions[i] for i in free]), rest
        for i in free:
            addition = min(bound - given[i], max(1, left * portions[i] // pool), rest)
            given[i] = given[i] + addition
            rest = rest - addition
    return np.array(given)


def centred(rng, dims, width, limit, cuts=(), kind=jnp.bfloat16):
    array = width * jax.random.normal(rng, dims, jnp.float32)
    if cuts:
        array = array * block_levels(rng, dims, cuts, -0.22, 0.18)
    return jnp.clip(array, -limit, limit).astype(kind)


def setup_inputs(seed: int = 0, part: int = 0) -> dict:
    key_list = jax.random.split(jax.random.key(seed), 9)
    part_splits = jax.random.split(jax.random.fold_in(key_list[8], part), 9)
    coarse_spectra = centred(part_splits[0], (SEGS, 2, FC), 1.0, 6.0, ((0, 8), (2, 2)))
    fine_spectra = centred(part_splits[1], (SEGS, 2, FB), 1.0, 6.0, ((0, 8), (2, 2)))
    coarse_templates = centred(key_list[2], (2, TC, FC), 1.0, 6.0, ((1, 4), (2, 2)))
    fine_templates = centred(key_list[3], (2, SUBBANKS, TSUB, FB), 1.0, 6.0, ((1, 4), (3, 2)))
    coarse_weight = jnp.clip(jnp.exp(math.log(2.0) - 2.3025851 * jax.random.uniform(part_splits[4], (FC,), jnp.float32) ** block_levels(part_splits[4], (FC,), ((0, 2),), -0.2, 0.2)), 0.2, 2.0)
    fine_weight = jnp.clip(jnp.exp(math.log(2.0) - 2.3025851 * jax.random.uniform(part_splits[5], (FB,), jnp.float32) ** block_levels(part_splits[5], (FB,), ((0, 2),), -0.2, 0.2)), 0.2, 2.0)
    triggers_keys = jax.random.split(jax.random.fold_in(part_splits[6], 1), SEGS // SEG_DEV)
    triggers_turns = jax.random.permutation(jax.random.fold_in(part_splits[6], 3), SEGS // SEG_DEV)
    triggers = jax.vmap(lambda own, number: shared_out(jax.random.fold_in(part_splits[6], 2), own, number, SEG_DEV, SUBBANKS, TOP, CAP, 2))(triggers_keys, triggers_turns).reshape((SEGS, TOP))
    offsets = place_ends(jax.random.randint(part_splits[7], (SEGS, TOP), 0, 2 * FB - LF + 1), jax.random.fold_in(part_splits[7], 1), 0, 2 * FB - LF).astype(jnp.int32)
    return dict(coarse_spectra=coarse_spectra, fine_spectra=fine_spectra, coarse_templates=coarse_templates, fine_templates=fine_templates, coarse_weight=coarse_weight, fine_weight=fine_weight, triggers=triggers, offsets=offsets)


def phase_of(counts, period):
    radians = (2.0 * math.pi / period) * counts.astype(jnp.float32)
    return jnp.cos(radians), jnp.sin(radians)


def offset_count(freq_ids, offset, period):
    upper_bits = offset // 512
    lower_bits = offset % 512
    lower_term = (freq_ids * lower_bits) % period
    upper_term = ((freq_ids * upper_bits) % (period // 512)) * 512
    return (lower_term + upper_term) % period


def lagged(real_part, imag_part, lag_cos, lag_sin):
    left_real = real_part.T[:, :, None]
    left_imag = imag_part.T[:, :, None]
    right_cos = lag_cos[:, None, :]
    right_sin = lag_sin[:, None, :]
    lag_real = (left_real * right_cos - left_imag * right_sin).astype(jnp.bfloat16)
    lag_imag = (left_real * right_sin + left_imag * right_cos).astype(jnp.bfloat16)
    columns = real_part.shape[0] * lag_cos.shape[1]
    return lag_real.reshape(-1, columns), lag_imag.reshape(-1, columns)


def correlate(temp_real, temp_imag, lag_real, lag_imag):
    corr_real = jnp.dot(temp_real, lag_real, preferred_element_type=jnp.float32) + jnp.dot(temp_imag, lag_imag, preferred_element_type=jnp.float32)
    corr_imag = jnp.dot(temp_real, lag_imag, preferred_element_type=jnp.float32) - jnp.dot(temp_imag, lag_real, preferred_element_type=jnp.float32)
    return corr_real, corr_imag


def reference(coarse_spectra, fine_spectra, coarse_templates, fine_templates, coarse_weight, fine_weight, triggers, offsets):
    period_coarse = 2 * FC
    coarse_ids = jnp.arange(FC, dtype=jnp.int32)
    coarse_lags = jnp.arange(LC, dtype=jnp.int32) * CSTRIDE
    coarse_cos, coarse_sin = phase_of((coarse_ids[:, None] * coarse_lags[None, :]) % period_coarse, period_coarse)
    temp_real = coarse_templates[0]
    temp_imag = coarse_templates[1]
    coarse_norm = jnp.sum((temp_real.astype(jnp.float32) ** 2 + temp_imag.astype(jnp.float32) ** 2) * coarse_weight[None, :], axis=1)
    segment_blocks = coarse_spectra.reshape(SEGS // 8, 8, 2, FC)

    def coarse_block(segment_block):
        weighted = segment_block.astype(jnp.float32) * coarse_weight[None, None, :]
        lag_real, lag_imag = lagged(weighted[:, 0], weighted[:, 1], coarse_cos, coarse_sin)
        corr_real, corr_imag = correlate(temp_real, temp_imag, lag_real, lag_imag)
        energy = (corr_real * corr_real + corr_imag * corr_imag).reshape(TC, 8, LC)
        return jnp.max(energy, axis=2)

    peaks = lax.map(coarse_block, segment_blocks)
    coarse_snr = jnp.transpose(peaks, (1, 0, 2)).reshape(TC, SEGS) / coarse_norm[:, None]

    period_fine = 2 * FB
    fine_ids = jnp.arange(FB, dtype=jnp.int32)
    fine_lags = jnp.arange(LF, dtype=jnp.int32)
    fine_cos, fine_sin = phase_of((fine_ids[:, None] * fine_lags[None, :]) % period_fine, period_fine)
    fine_norm = jnp.sum((fine_templates[0].astype(jnp.float32) ** 2 + fine_templates[1].astype(jnp.float32) ** 2) * fine_weight[None, None, :], axis=2)
    pair_segments = jnp.repeat(jnp.arange(SEGS, dtype=jnp.int32), TOP)

    def fine_pair(pair):
        segment_id, bank_id, offset = pair
        spectrum = lax.dynamic_index_in_dim(fine_spectra, segment_id, 0, keepdims=False).astype(jnp.float32) * fine_weight[None, :]
        shift_cos, shift_sin = phase_of(offset_count(fine_ids, offset, period_fine), period_fine)
        shifted_real = spectrum[0] * shift_cos - spectrum[1] * shift_sin
        shifted_imag = spectrum[0] * shift_sin + spectrum[1] * shift_cos
        lag_real, lag_imag = lagged(shifted_real[None, :], shifted_imag[None, :], fine_cos, fine_sin)
        chosen = lax.dynamic_index_in_dim(fine_templates, bank_id, 1, keepdims=False)
        corr_real, corr_imag = correlate(chosen[0], chosen[1], lag_real, lag_imag)
        norm_row = lax.dynamic_index_in_dim(fine_norm, bank_id, 0, keepdims=False)
        return jnp.max(corr_real * corr_real + corr_imag * corr_imag, axis=1) / norm_row

    fine_rows = lax.map(fine_pair, (pair_segments, triggers.reshape(-1).astype(jnp.int32), offsets.reshape(-1).astype(jnp.int32)))
    return coarse_snr, fine_rows.reshape(SEGS, TOP, TSUB)
```

```python
import functools
import math

import jax
import jax.numpy as jnp
from jax import lax
from jax.experimental import pallas as pl
from jax.experimental.pallas import tpu as pltpu
from jax.sharding import PartitionSpec as P

CAP = 2
LAGS = 16
PAIRS = LAGS // 2
CSTRIDE = 2047
LANES = 128
F32 = jnp.float32
BF16 = jnp.bfloat16
VMEM_LIMIT = 48 * 1024 * 1024


def sincos(counts, period):
    half = period // 2
    signed = ((counts + half) & (period - 1)) - half
    x = signed.astype(F32) * (1.0 / period)
    u = x * x
    p = math.pi
    s = -(p**11) / 39916800.0
    for a in (p**9 / 362880.0, -(p**7) / 5040.0, p**5 / 120.0, -(p**3) / 6.0, p):
        s = s * u + a
    s = s * x
    c = p**12 / 479001600.0
    for a in (-(p**10) / 3628800.0, p**8 / 40320.0, -(p**6) / 720.0, p**4 / 24.0, -(p**2) / 2.0, 1.0):
        c = c * u + a
    return 1.0 - 2.0 * s * s, 2.0 * s * c


def dot_t(a, b):
    return lax.dot_general(a, b, (((1,), (1,)), ((), ())), preferred_element_type=F32)


def rotate(c, s, dc, ds):
    return c * dc - s * ds, s * dc + c * ds


def coarse_kernel(
    info_ref, w_ref, h_ref, *rest, blocks, segs, banks, freqs, steps, kc, period
):
    spec_refs = rest[:blocks]
    keep_ref, keepn_ref, send_ref = rest[blocks : blocks + 3]
    a_ref, b_ref, y_ref, acc_ref, nacc_ref, tab_ref, ctr_ref = rest[blocks + 3 :]
    step = pl.program_id(0)
    base = info_ref[0]
    bank = info_ref[1]
    freq = info_ref[2]
    total = banks * segs
    cols = total * LAGS

    @pl.when(step == 0)
    def _():
        ids = base + lax.broadcasted_iota(jnp.int32, (PAIRS, kc), 1)
        odd = 2 * lax.broadcasted_iota(jnp.int32, (PAIRS, kc), 0) + 1
        c, s = sincos(ids * odd * CSTRIDE, period)
        tab_ref[0] = c
        tab_ref[1] = s
        c, s = sincos(ids * (15 * CSTRIDE), period)
        ctr_ref[0] = c
        ctr_ref[1] = s
        acc_ref[...] = jnp.zeros_like(acc_ref)
        nacc_ref[...] = jnp.zeros_like(nacc_ref)

    w = w_ref[...]
    for k in range(blocks):
        source = lax.rem(bank - k + banks, banks)
        for i in range(segs):
            a_ref[source, 2 * i : 2 * i + 2, :] = spec_refs[k][i].astype(F32) * w

    shift = step * kc
    odd = 2 * lax.broadcasted_iota(jnp.int32, (PAIRS, LANES), 0) + 1
    dc, ds = sincos(shift * odd * CSTRIDE, period)
    ec, es = sincos(jnp.full((PAIRS, LANES), shift * (15 * CSTRIDE), jnp.int32), period)
    for lo in range(0, kc, LANES):
        lanes = slice(lo, lo + LANES)
        c, s = rotate(ctr_ref[0, :, lanes], ctr_ref[1, :, lanes], ec, es)
        for b in range(0, total, 4):
            re = jnp.concatenate(
                [a_ref[(b + i) // segs, 2 * ((b + i) % segs) : 2 * ((b + i) % segs) + 1, lanes] for i in range(4)], axis=0
            )
            im = jnp.concatenate(
                [a_ref[(b + i) // segs, 2 * ((b + i) % segs) + 1 : 2 * ((b + i) % segs) + 2, lanes] for i in range(4)], axis=0
            )
            b_ref[0, b : b + 4, lanes] = re * c[:4] - im * s[:4]
            b_ref[1, b : b + 4, lanes] = re * s[:4] + im * c[:4]
        c, s = rotate(tab_ref[0, :, lanes], tab_ref[1, :, lanes], dc, ds)
        tab_ref[2, :, lanes] = c
        tab_ref[3, :, lanes] = s
        re = b_ref[0, :, lanes]
        im = b_ref[1, :, lanes]
        for m in range(PAIRS):
            cm = tab_ref[2, m : m + 1, lanes]
            sm = tab_ref[3, m : m + 1, lanes]
            rc = re * cm
            js = im * sm
            jc = im * cm
            rs = re * sm
            for sign, (yr, yi) in enumerate(((rc - js, jc + rs), (rc + js, jc - rs))):
                at = (2 * m + sign) * total
                yr = yr.astype(BF16)
                yi = yi.astype(BF16)
                y_ref[at : at + total, lo : lo + LANES] = yr
                y_ref[at : at + total, kc + lo : kc + lo + LANES] = yi
                y_ref[cols + at : cols + at + total, lo : lo + LANES] = yi
                y_ref[cols + at : cols + at + total, kc + lo : kc + lo + LANES] = -yr

    acc_ref[...] += dot_t(jnp.concatenate([h_ref[0], h_ref[1]], axis=1), y_ref[...])
    rows = acc_ref.shape[0]
    chunk = min(rows, 64)
    for r in range(0, rows, chunk):
        n = nacc_ref[r : r + chunk, :]
        for lo in range(0, kc, LANES):
            hr = h_ref[0, r : r + chunk, lo : lo + LANES].astype(F32)
            hi = h_ref[1, r : r + chunk, lo : lo + LANES].astype(F32)
            n = n + (hr * hr + hi * hi) * w[:, lo : lo + LANES]
        nacc_ref[r : r + chunk, :] = n

    @pl.when(step == steps - 1)
    def _():
        part = rows // freqs
        own = pl.multiple_of(freq * part, part)
        keep_ref[...] = acc_ref[pl.ds(own, part), :]
        keepn_ref[...] = jnp.broadcast_to(
            jnp.sum(nacc_ref[pl.ds(own, part), :], axis=1, keepdims=True), (part, LANES)
        )
        for k in range(1, freqs):
            dest = pl.multiple_of(lax.rem(freq + k, freqs) * part, part)
            send_ref[k - 1, :part, :] = acc_ref[pl.ds(dest, part), :].astype(BF16)
            send_ref[k - 1, part:, :] = jnp.zeros((16, 2 * cols), BF16)
            for r in range(0, part, min(part, LANES)):
                size = min(part, LANES)
                n = nacc_ref[pl.ds(dest + r, size), :]
                if size < LANES:
                    n = jnp.concatenate([n, jnp.zeros((LANES - size, LANES), F32)], axis=0)
                n = jnp.sum(n.T, axis=0, keepdims=True)
                high = n.astype(BF16).astype(F32)
                low = n - high
                row = lax.broadcasted_iota(jnp.int32, (16, LANES), 0)
                send_ref[k - 1, part : part + 16, r : r + LANES] = jnp.where(
                    row == 0, high, jnp.where(row == 1, low, 0.0)
                ).astype(BF16)


def coarse_final_kernel(keep_ref, keepn_ref, *rest, freqs, total):
    recv_refs = rest[: freqs - 1]
    out_ref = rest[freqs - 1]
    part = keep_ref.shape[0]
    cols = total * LAGS
    corr = keep_ref[...]
    norm = keepn_ref[:, 0:1]
    size = min(part, LANES)
    for ref in recv_refs:
        corr = corr + ref[0, :part, :].astype(F32)
        pieces = []
        for r in range(0, part, size):
            n = jnp.sum(ref[0, part : part + 16, r : r + LANES].astype(F32), axis=0, keepdims=True)
            pieces.append(jnp.broadcast_to(n, (LANES, LANES)).T[:size, 0:1])
        norm = norm + (jnp.concatenate(pieces, axis=0) if len(pieces) > 1 else pieces[0])
    cr = corr[:, :cols]
    ci = corr[:, cols:]
    e = cr * cr + ci * ci
    width = cols
    while width > max(total, LANES):
        width //= 2
        e = jnp.maximum(e[:, :width], e[:, width:])
    while width > total:
        width //= 2
        e = jnp.maximum(e, pltpu.roll(e, LANES - width, 1))
    out_ref[...] = (e / norm)[:, :total]


def fine_kernel(info_ref, w_ref, mult_ref, g_ref, *rest, blocks, freqs, steps, kc, period):
    slot_refs = rest[:blocks]
    keep_ref, send_ref = rest[blocks : blocks + 2]
    a_ref, b_ref, y_ref, acc_ref, nacc_ref, tab_ref, ctr_ref = rest[blocks + 2 :]
    step = pl.program_id(0)
    base = info_ref[0]
    freq = info_ref[2]
    n = blocks * CAP
    cols = n * LAGS
    tsub = g_ref.shape[2]

    @pl.when(step == 0)
    def _():
        ids = base + lax.broadcasted_iota(jnp.int32, (PAIRS, kc), 1)
        odd = 2 * lax.broadcasted_iota(jnp.int32, (PAIRS, kc), 0) + 1
        c, s = sincos(ids * odd, period)
        tab_ref[0] = c
        tab_ref[1] = s
        ids = base + lax.broadcasted_iota(jnp.int32, (n, kc), 1)
        c, s = sincos(ids * mult_ref[:, 0:1], period)
        ctr_ref[0] = c
        ctr_ref[1] = s
        acc_ref[...] = jnp.zeros_like(acc_ref)
        nacc_ref[...] = jnp.zeros_like(nacc_ref)

    w = w_ref[...]
    for k in range(blocks):
        for i in range(CAP):
            x = slot_refs[k][i].astype(F32) * w
            a_ref[0, CAP * k + i : CAP * k + i + 1, :] = x[0:1]
            a_ref[1, CAP * k + i : CAP * k + i + 1, :] = x[1:2]

    shift = step * kc
    odd = 2 * lax.broadcasted_iota(jnp.int32, (PAIRS, LANES), 0) + 1
    dc, ds = sincos(shift * odd, period)
    ec, es = sincos(shift * mult_ref[...], period)
    for lo in range(0, kc, LANES):
        lanes = slice(lo, lo + LANES)
        c, s = rotate(ctr_ref[0, :, lanes], ctr_ref[1, :, lanes], ec, es)
        re = a_ref[0, :, lanes]
        im = a_ref[1, :, lanes]
        b_ref[0, :, lanes] = re * c - im * s
        b_ref[1, :, lanes] = re * s + im * c
        c, s = rotate(tab_ref[0, :, lanes], tab_ref[1, :, lanes], dc, ds)
        for i in range(n):
            re = b_ref[0, i : i + 1, lanes]
            im = b_ref[1, i : i + 1, lanes]
            rc = re * c
            js = im * s
            jc = im * c
            rs = re * s
            at = i * LAGS
            y_ref[at : at + LAGS, lanes] = jnp.concatenate([rc - js, rc + js], axis=0).astype(BF16)
            y_ref[cols + at : cols + at + LAGS, lanes] = jnp.concatenate(
                [jc + rs, jc - rs], axis=0
            ).astype(BF16)

    g = jnp.concatenate([g_ref[0, 0], g_ref[1, 0]], axis=0)
    acc_ref[...] += dot_t(y_ref[...], g)
    norm = nacc_ref[...]
    for lo in range(0, kc, LANES):
        gr = g_ref[0, 0, :, lo : lo + LANES].astype(F32)
        gi = g_ref[1, 0, :, lo : lo + LANES].astype(F32)
        norm = norm + (gr * gr + gi * gi) * w[:, lo : lo + LANES]
    nacc_ref[...] = norm

    @pl.when(step == steps - 1)
    def _():
        part = tsub // freqs
        acc = acc_ref[...]
        swap = pltpu.roll(acc, LANES - tsub, 1)
        corr_real = acc[:cols] + swap[cols:]
        corr_imag = acc[cols:] - swap[:cols]
        norms = jnp.concatenate([nacc_ref[...], jnp.zeros((LANES - tsub, LANES), F32)], axis=0)
        norms = jnp.sum(norms.T, axis=0, keepdims=True)
        norms = jnp.broadcast_to(norms, (8, LANES))
        lane = lax.broadcasted_iota(jnp.int32, (1, LANES), 1)

        def pack(dest):
            real, imag, norm_row = corr_real, corr_imag, norms
            out_real, out_imag, out_norm = real, pltpu.roll(imag, part, 1), norm_row
            for d in range(1, freqs):
                here = dest == d
                out_real = jnp.where(here, pltpu.roll(real, LANES - d * part, 1), out_real)
                out_imag = jnp.where(here, pltpu.roll(imag, (LANES + part - d * part) % LANES, 1) if d != 1 else imag, out_imag)
                out_norm = jnp.where(here, pltpu.roll(norm_row, LANES - d * part, 1), out_norm)
            return jnp.concatenate(
                [jnp.where(lane < part, out_real, jnp.where(lane < 2 * part, out_imag, 0.0)), out_norm], axis=0
            )

        keep_ref[...] = pack(freq)
        for k in range(1, freqs):
            send_ref[k - 1] = pack(lax.rem(freq + k, freqs))


def fine_final_kernel(keep_ref, *rest, freqs, n, part):
    recv_refs = rest[: freqs - 1]
    out_ref = rest[freqs - 1]
    x = keep_ref[...]
    for ref in recv_refs:
        x = x + ref[0]
    norm = x[n * LAGS : n * LAGS + 1]
    e = x[: n * LAGS]
    e = e * e
    e = e + pltpu.roll(e, LANES - part, 1)
    rows = [jnp.max(e[i * LAGS : (i + 1) * LAGS], axis=0, keepdims=True) for i in range(n)]
    out_ref[...] = jnp.concatenate(rows, axis=0) / norm


def vmem_spec():
    return pl.BlockSpec(memory_space=pltpu.VMEM)


def params(**kw):
    return pltpu.CompilerParams(vmem_limit_bytes=VMEM_LIMIT, **kw)


def coarse_section(info, weight, templates, blocks, banks, freqs, period):
    segs = blocks[0].shape[0]
    rows, bins = templates.shape[1], templates.shape[2]
    total = banks * segs
    cols = total * LAGS
    kc = min(1024, bins)
    steps = bins // kc
    part = rows // freqs
    kernel = functools.partial(
        coarse_kernel, blocks=len(blocks), segs=segs, banks=banks, freqs=freqs, steps=steps, kc=kc, period=period
    )
    return pl.pallas_call(
        kernel,
        grid=(steps,),
        in_specs=[
            pl.BlockSpec(memory_space=pltpu.SMEM),
            pl.BlockSpec((1, kc), lambda i: (0, i)),
            pl.BlockSpec((2, rows, kc), lambda i: (0, 0, i)),
        ]
        + [pl.BlockSpec((segs, 2, kc), lambda i: (0, 0, i)) for _ in blocks],
        out_specs=[
            pl.BlockSpec((part, 2 * cols), lambda i: (0, 0)),
            pl.BlockSpec((part, LANES), lambda i: (0, 0)),
            pl.BlockSpec((freqs - 1, part + 16, 2 * cols), lambda i: (0, 0, 0)),
        ],
        out_shape=[
            jax.ShapeDtypeStruct((part, 2 * cols), F32),
            jax.ShapeDtypeStruct((part, LANES), F32),
            jax.ShapeDtypeStruct((freqs - 1, part + 16, 2 * cols), BF16),
        ],
        scratch_shapes=[
            pltpu.VMEM((banks, 2 * segs, kc), F32),
            pltpu.VMEM((2, total, kc), F32),
            pltpu.VMEM((2 * cols, 2 * kc), BF16),
            pltpu.VMEM((rows, 2 * cols), F32),
            pltpu.VMEM((rows, LANES), F32),
            pltpu.VMEM((4, PAIRS, kc), F32),
            pltpu.VMEM((2, PAIRS, kc), F32),
        ],
        compiler_params=params(dimension_semantics=("arbitrary",)),
        cost_estimate=pl.CostEstimate(
            flops=8 * rows * bins * cols, bytes_accessed=4 * rows * bins, transcendentals=0
        ),
        name="coarse",
    )(info, weight, templates, *blocks)


def fine_section(info, weight, mult, templates, blocks, freqs, period):
    bins = templates.shape[3]
    tsub = templates.shape[2]
    n = CAP * len(blocks)
    cols = n * LAGS
    kc = min(4096, bins)
    steps = bins // kc
    kernel = functools.partial(
        fine_kernel, blocks=len(blocks), freqs=freqs, steps=steps, kc=kc, period=period
    )
    return pl.pallas_call(
        kernel,
        grid=(steps,),
        in_specs=[
            pl.BlockSpec(memory_space=pltpu.SMEM),
            pl.BlockSpec((1, kc), lambda i: (0, i)),
            pl.BlockSpec((n, LANES), lambda i: (0, 0)),
            pl.BlockSpec((2, 1, tsub, kc), lambda i: (0, 0, 0, i)),
        ]
        + [pl.BlockSpec((CAP, 2, kc), lambda i: (0, 0, i)) for _ in blocks],
        out_specs=[
            pl.BlockSpec((cols + 8, LANES), lambda i: (0, 0)),
            pl.BlockSpec((freqs - 1, cols + 8, LANES), lambda i: (0, 0, 0)),
        ],
        out_shape=[
            jax.ShapeDtypeStruct((cols + 8, LANES), F32),
            jax.ShapeDtypeStruct((freqs - 1, cols + 8, LANES), F32),
        ],
        scratch_shapes=[
            pltpu.VMEM((2, n, kc), F32),
            pltpu.VMEM((2, n, kc), F32),
            pltpu.VMEM((2 * cols, kc), BF16),
            pltpu.VMEM((2 * cols, LANES), F32),
            pltpu.VMEM((tsub, LANES), F32),
            pltpu.VMEM((2, PAIRS, kc), F32),
            pltpu.VMEM((2, n, kc), F32),
        ],
        compiler_params=params(dimension_semantics=("arbitrary",)),
        cost_estimate=pl.CostEstimate(
            flops=8 * tsub * bins * cols, bytes_accessed=4 * tsub * bins, transcendentals=0
        ),
        name="fine",
    )(info, weight, mult, templates, *blocks)


def shift_permute(value, axis, count, by):
    return lax.ppermute(value, axis, [(i, (i + by) % count) for i in range(count)])


def pair_slots(naming):
    ranking = jnp.cumsum(naming.astype(jnp.int32), axis=1) - 1
    columns = jnp.arange(CAP, dtype=jnp.int32)
    return naming[:, None, :] & (ranking[:, None, :] == columns[None, :, None])


def body(
    coarse_spectra,
    fine_spectra,
    coarse_templates,
    fine_templates,
    coarse_weight,
    fine_weight,
    triggers,
    offsets,
):
    banks = lax.axis_size("bank")
    freqs = lax.axis_size("freq")
    bank = lax.axis_index("bank")
    freq = lax.axis_index("freq")
    segs = fine_spectra.shape[0]
    coarse_bins = coarse_spectra.shape[2]
    fine_bins = fine_spectra.shape[2]
    top = triggers.shape[1]
    tsub = fine_templates.shape[2]
    part = tsub // freqs
    coarse_period = 4 * coarse_bins * freqs
    fine_period = 4 * fine_bins * freqs
    zero = jnp.zeros((), jnp.int32)
    coarse_info = jnp.stack([freq * coarse_bins, bank, freq, zero]).astype(jnp.int32)
    fine_info = jnp.stack([freq * fine_bins, bank, freq, zero]).astype(jnp.int32)

    coarse_blocks = [coarse_spectra] + [
        shift_permute(coarse_spectra, "bank", banks, k) for k in range(1, banks)
    ]

    trig_blocks = triggers.reshape(banks, segs * top)
    offset_blocks = offsets.reshape(banks, segs * top)
    recv_pairs = pair_slots(trig_blocks == bank)
    slot_offsets = jnp.sum(jnp.where(recv_pairs, offset_blocks[:, None, :], 0), axis=2)
    mult = jnp.broadcast_to((2 * slot_offsets + (LAGS - 1))[:, :, None], (banks, CAP, LANES))
    own_pairs = lax.dynamic_index_in_dim(trig_blocks, bank, 0, keepdims=False)
    targets = jnp.arange(banks, dtype=jnp.int32)
    send_pairs = pair_slots(own_pairs[None, :] == targets[:, None])
    pair_segment = jnp.arange(segs * top, dtype=jnp.int32) // top
    send_segment = jnp.sum(jnp.where(send_pairs, pair_segment[None, None, :], 0), axis=2)

    fine_blocks = []
    block_mult = []
    for k in range(banks):
        dest = lax.rem(bank + k, banks)
        chosen = lax.dynamic_index_in_dim(send_segment, dest, 0, keepdims=False)
        picked = jnp.concatenate(
            [lax.dynamic_slice_in_dim(fine_spectra, chosen[c], 1, 0) for c in range(CAP)], axis=0
        )
        fine_blocks.append(picked if k == 0 else shift_permute(picked, "bank", banks, k))
        source = lax.rem(bank - k + banks, banks)
        block_mult.append(lax.dynamic_index_in_dim(mult, source, 0, keepdims=False))

    keep, keep_norm, send = coarse_section(
        coarse_info,
        coarse_weight.reshape(1, -1),
        coarse_templates,
        coarse_blocks,
        banks,
        freqs,
        coarse_period,
    )
    received = [shift_permute(send[k - 1 : k], "freq", freqs, k) for k in range(1, freqs)]
    coarse_snr = pl.pallas_call(
        functools.partial(coarse_final_kernel, freqs=freqs, total=banks * segs),
        out_shape=jax.ShapeDtypeStruct((keep.shape[0], banks * segs), F32),
        compiler_params=params(),
        name="coarse_final",
    )(keep, keep_norm, *received)

    keep, send = fine_section(
        fine_info,
        fine_weight.reshape(1, -1),
        jnp.concatenate(block_mult, axis=0),
        fine_templates,
        fine_blocks,
        freqs,
        fine_period,
    )
    received = [shift_permute(send[k - 1 : k], "freq", freqs, k) for k in range(1, freqs)]
    n = CAP * banks
    slot_snr = pl.pallas_call(
        functools.partial(fine_final_kernel, freqs=freqs, n=n, part=part),
        out_shape=jax.ShapeDtypeStruct((n, LANES), F32),
        compiler_params=params(),
        name="fine_final",
    )(keep, *received)
    slot_snr = slot_snr.reshape(banks, CAP, LANES)
    rows = jnp.zeros((segs * top, LANES), F32)
    for k in range(banks):
        back = slot_snr[k] if k == 0 else shift_permute(slot_snr[k], "bank", banks, banks - k)
        owner = lax.rem(bank + k, banks)
        select = lax.dynamic_index_in_dim(send_pairs, owner, 0, keepdims=False)
        rows = rows + jnp.sum(jnp.where(select[:, :, None], back[:, None, :], 0.0), axis=0)
    fine_snr = rows[:, :part].reshape(segs, top, part)
    return (coarse_snr, fine_snr)


def solution(mesh):
    return jax.shard_map(
        body,
        mesh=mesh,
        in_specs=(
            P(("groups", "seg", "bank"), None, "freq"),
            P(("groups", "seg", "bank"), None, "freq"),
            P(None, "bank", "freq"),
            P(None, "bank", None, "freq"),
            P(("groups", "freq")),
            P(("groups", "freq")),
            P(("groups", "seg"), None),
            P(("groups", "seg"), None),
        ),
        out_specs=(
            P(("bank", "freq"), ("groups", "seg")),
            P(("groups", "seg", "bank"), None, "freq"),
        ),
        check_vma=False,
    )
```

```python
import functools
import math

import jax
import jax.numpy as jnp
from jax import lax
from jax.experimental import pallas as pl
from jax.experimental.pallas import tpu as pltpu
from jax.sharding import PartitionSpec as P

CAP = 2
LAGS = 16
PAIRS = LAGS // 2
CSTRIDE = 2047
LANES = 128
F32 = jnp.float32
BF16 = jnp.bfloat16


def sincos(counts, period):
    half = period // 2
    signed = ((counts + half) & (period - 1)) - half
    x = signed.astype(F32) * (1.0 / period)
    u = x * x
    p = math.pi
    s = -(p**11) / 39916800.0
    for a in (p**9 / 362880.0, -(p**7) / 5040.0, p**5 / 120.0, -(p**3) / 6.0, p):
        s = s * u + a
    s = s * x
    c = p**12 / 479001600.0
    for a in (-(p**10) / 3628800.0, p**8 / 40320.0, -(p**6) / 720.0, p**4 / 24.0, -(p**2) / 2.0, 1.0):
        c = c * u + a
    return 1.0 - 2.0 * s * s, 2.0 * s * c


def dot_t(a, b):
    return lax.dot_general(a, b, (((1,), (1,)), ((), ())), preferred_element_type=F32)


def rotate(c, s, dc, ds):
    return c * dc - s * ds, s * dc + c * ds


def coarse_kernel(
    info_ref, w_ref, h_ref, *rest, blocks, segs, banks, freqs, steps, kc, period
):
    spec_refs = rest[:blocks]
    keep_ref, send_ref = rest[blocks : blocks + 2]
    a_ref, b_ref, y_ref, acc_ref, tab_ref, ctr_ref = rest[blocks + 2 :]
    step = pl.program_id(0)
    base = info_ref[0]
    bank = info_ref[1]
    freq = info_ref[2]
    total = banks * segs
    cols = total * LAGS

    @pl.when(step == 0)
    def _():
        ids = base + lax.broadcasted_iota(jnp.int32, (PAIRS, kc), 1)
        odd = 2 * lax.broadcasted_iota(jnp.int32, (PAIRS, kc), 0) + 1
        c, s = sincos(ids * odd * CSTRIDE, period)
        tab_ref[0] = c
        tab_ref[1] = s
        c, s = sincos(ids * (15 * CSTRIDE), period)
        ctr_ref[0] = c
        ctr_ref[1] = s
        acc_ref[...] = jnp.zeros_like(acc_ref)

    w = w_ref[...]
    for k in range(blocks):
        source = lax.rem(bank - k + banks, banks)
        for i in range(segs):
            a_ref[source, 2 * i : 2 * i + 2, :] = spec_refs[k][i].astype(F32) * w

    shift = step * kc
    odd = 2 * lax.broadcasted_iota(jnp.int32, (PAIRS, LANES), 0) + 1
    dc, ds = sincos(shift * odd * CSTRIDE, period)
    ec, es = sincos(jnp.full((PAIRS, LANES), shift * (15 * CSTRIDE), jnp.int32), period)
    for lo in range(0, kc, LANES):
        lanes = slice(lo, lo + LANES)
        c, s = rotate(ctr_ref[0, :, lanes], ctr_ref[1, :, lanes], ec, es)
        for b in range(0, total, 4):
            re = jnp.concatenate(
                [a_ref[(b + i) // segs, 2 * ((b + i) % segs) : 2 * ((b + i) % segs) + 1, lanes] for i in range(4)], axis=0
            )
            im = jnp.concatenate(
                [a_ref[(b + i) // segs, 2 * ((b + i) % segs) + 1 : 2 * ((b + i) % segs) + 2, lanes] for i in range(4)], axis=0
            )
            b_ref[0, b : b + 4, lanes] = re * c[:4] - im * s[:4]
            b_ref[1, b : b + 4, lanes] = re * s[:4] + im * c[:4]
        c, s = rotate(tab_ref[0, :, lanes], tab_ref[1, :, lanes], dc, ds)
        tab_ref[2, :, lanes] = c
        tab_ref[3, :, lanes] = s
        re = b_ref[0, :, lanes]
        im = b_ref[1, :, lanes]
        for m in range(PAIRS):
            cm = tab_ref[2, m : m + 1, lanes]
            sm = tab_ref[3, m : m + 1, lanes]
            rc = re * cm
            js = im * sm
            jc = im * cm
            rs = re * sm
            for sign, (yr, yi) in enumerate(((rc - js, jc + rs), (rc + js, jc - rs))):
                at = (2 * m + sign) * total
                yr = yr.astype(BF16)
                yi = yi.astype(BF16)
                y_ref[at : at + total, lo : lo + LANES] = yr
                y_ref[at : at + total, kc + lo : kc + lo + LANES] = yi
                y_ref[cols + at : cols + at + total, lo : lo + LANES] = yi
                y_ref[cols + at : cols + at + total, kc + lo : kc + lo + LANES] = -yr

    acc_ref[...] += dot_t(jnp.concatenate([h_ref[0], h_ref[1]], axis=1), y_ref[...])

    @pl.when(step == steps - 1)
    def _():
        part = acc_ref.shape[0] // freqs
        own = pl.multiple_of(freq * part, part)
        keep_ref[...] = acc_ref[pl.ds(own, part), :]
        for k in range(1, freqs):
            dest = pl.multiple_of(lax.rem(freq + k, freqs) * part, part)
            send_ref[k - 1] = acc_ref[pl.ds(dest, part), :]


def coarse_final_kernel(keep_ref, norm_ref, *rest, freqs, total):
    recv_refs = rest[: 2 * (freqs - 1)]
    out_ref = rest[2 * (freqs - 1)]
    part = keep_ref.shape[0]
    cols = total * LAGS
    corr = keep_ref[...]
    norms = norm_ref[...]
    for k in range(freqs - 1):
        corr = corr + recv_refs[2 * k][0]
        norms = norms + recv_refs[2 * k + 1][0]
    cr = corr[:, :cols]
    ci = corr[:, cols:]
    e = cr * cr + ci * ci
    width = cols
    while width > max(total, LANES):
        width //= 2
        e = jnp.maximum(e[:, :width], e[:, width:])
    while width > total:
        width //= 2
        e = jnp.maximum(e, pltpu.roll(e, LANES - width, 1))
    size = min(part, LANES)
    for r in range(part // size):
        rows = e[r * size : (r + 1) * size]
        if size < LANES:
            rows = jnp.concatenate([rows, jnp.zeros((LANES - size, LANES), F32)], axis=0)
        out = rows.T[:total] / norms[r : r + 1]
        out_ref[:, r * size : (r + 1) * size] = out[:, :size]


def norm_kernel(info_ref, cw_ref, fw_ref, h_ref, g_ref, keep_ref, send_ref, c_ref, f_ref, *, freqs, steps):
    step = pl.program_id(0)

    @pl.when(step == 0)
    def _():
        c_ref[...] = jnp.zeros_like(c_ref)
        f_ref[...] = jnp.zeros_like(f_ref)

    def add(acc_ref, w_ref, load, rows, bins):
        chunk = min(rows, 64)
        w = w_ref[...]
        for r in range(0, rows, chunk):
            n = acc_ref[r : r + chunk, :]
            for lo in range(0, bins, LANES):
                re = load(0, r, chunk, lo).astype(F32)
                im = load(1, r, chunk, lo).astype(F32)
                n = n + (re * re + im * im) * w[:, lo : lo + LANES]
            acc_ref[r : r + chunk, :] = n

    rows = h_ref.shape[1]
    tsub = g_ref.shape[2]
    add(c_ref, cw_ref, lambda c, r, n, lo: h_ref[c, r : r + n, lo : lo + LANES], rows, h_ref.shape[2])
    add(f_ref, fw_ref, lambda c, r, n, lo: g_ref[c, 0, r : r + n, lo : lo + LANES], tsub, g_ref.shape[3])

    @pl.when(step == steps - 1)
    def _():
        part = rows // freqs
        fine_part = tsub // freqs
        size = min(part, LANES)
        count = part // size

        def row(n):
            if n.shape[0] < LANES:
                n = jnp.concatenate([n, jnp.zeros((LANES - n.shape[0], LANES), F32)], axis=0)
            return jnp.sum(n.T, axis=0, keepdims=True)

        def lay(dest):
            first = pl.multiple_of(dest * part, part)
            lines = [row(c_ref[pl.ds(first + r * size, size), :]) for r in range(count)]
            lines.append(row(f_ref[pl.ds(pl.multiple_of(dest * fine_part, fine_part), fine_part), :]))
            lines.append(jnp.zeros((keep_ref.shape[0] - count - 1, LANES), F32))
            return jnp.concatenate(lines, axis=0)

        keep_ref[...] = lay(info_ref[2])
        for k in range(1, freqs):
            send_ref[k - 1] = lay(lax.rem(info_ref[2] + k, freqs))


def ranked_pairs(trig_ref, first, segs, top, target):
    taken = jnp.int32(0)
    found = [jnp.int32(0) for _ in range(CAP)]
    for p in range(segs * top):
        hit = (trig_ref[first + p // top, p % top] == target).astype(jnp.int32)
        for c in range(CAP):
            found[c] = jnp.where(jnp.logical_and(hit == 1, taken == c), p, found[c])
        taken = taken + hit
    return taken, found


def pick_kernel(info_ref, trig_ref, off_ref, spec_ref, *rest, banks, segs, top):
    out_refs = rest[:banks]
    mult_ref, sems = rest[banks:]
    bank = info_ref[1]
    copies = []
    for k in range(banks):
        k = (k + 1) % banks
        dest = lax.rem(bank + k, banks)
        _, found = ranked_pairs(trig_ref, bank * segs, segs, top, dest)
        for c in range(CAP):
            copy = pltpu.make_async_copy(
                spec_ref.at[found[c] // top], out_refs[k].at[c], sems.at[k * CAP + c]
            )
            copy.start()
            copies.append(copy)
    line = lax.broadcasted_iota(jnp.int32, mult_ref.shape, 0)
    mult = jnp.zeros(mult_ref.shape, jnp.int32)
    for k in range(banks):
        source = lax.rem(bank - k + banks, banks)
        taken, found = ranked_pairs(trig_ref, source * segs, segs, top, bank)
        for c in range(CAP):
            offset = off_ref[source * segs + found[c] // top, lax.rem(found[c], top)]
            mult = jnp.where(line == k * CAP + c, 2 * offset + (LAGS - 1), mult)
    mult_ref[...] = mult
    for copy in copies:
        copy.wait()


def place_kernel(info_ref, trig_ref, *rest, banks, segs, top):
    back_refs = rest[:banks]
    out_ref, all_ref = rest[banks:]
    bank = info_ref[1]
    part = out_ref.shape[2]
    for k in range(banks):
        all_ref[CAP * k : CAP * (k + 1), :] = back_refs[k][...]
    for p in range(segs * top):
        target = trig_ref[bank * segs + p // top, p % top]
        rank = jnp.int32(0)
        for q in range(p):
            rank = rank + (trig_ref[bank * segs + q // top, q % top] == target).astype(jnp.int32)
        at = lax.rem(target - bank + banks, banks) * CAP + jnp.minimum(rank, CAP - 1)
        out_ref[p // top, p % top : p % top + 1, :] = all_ref[pl.ds(at, 1), :][:, :part]


def fine_kernel(info_ref, w_ref, mult_ref, g_ref, *rest, blocks, freqs, steps, kc, period):
    slot_refs = rest[:blocks]
    keep_ref, send_ref = rest[blocks : blocks + 2]
    a_ref, b_ref, y_ref, acc_ref, tab_ref, ctr_ref = rest[blocks + 2 :]
    step = pl.program_id(0)
    base = info_ref[0]
    freq = info_ref[2]
    n = blocks * CAP
    cols = n * LAGS
    tsub = g_ref.shape[2]

    @pl.when(step == 0)
    def _():
        ids = base + lax.broadcasted_iota(jnp.int32, (PAIRS, kc), 1)
        odd = 2 * lax.broadcasted_iota(jnp.int32, (PAIRS, kc), 0) + 1
        c, s = sincos(ids * odd, period)
        tab_ref[0] = c
        tab_ref[1] = s
        ids = base + lax.broadcasted_iota(jnp.int32, (n, kc), 1)
        c, s = sincos(ids * mult_ref[:, 0:1], period)
        ctr_ref[0] = c
        ctr_ref[1] = s
        acc_ref[...] = jnp.zeros_like(acc_ref)

    w = w_ref[...]
    for k in range(blocks):
        for i in range(CAP):
            x = slot_refs[k][i].astype(F32) * w
            a_ref[0, CAP * k + i : CAP * k + i + 1, :] = x[0:1]
            a_ref[1, CAP * k + i : CAP * k + i + 1, :] = x[1:2]

    shift = step * kc
    odd = 2 * lax.broadcasted_iota(jnp.int32, (PAIRS, LANES), 0) + 1
    dc, ds = sincos(shift * odd, period)
    ec, es = sincos(shift * mult_ref[...], period)
    for lo in range(0, kc, LANES):
        lanes = slice(lo, lo + LANES)
        c, s = rotate(ctr_ref[0, :, lanes], ctr_ref[1, :, lanes], ec, es)
        re = a_ref[0, :, lanes]
        im = a_ref[1, :, lanes]
        b_ref[0, :, lanes] = re * c - im * s
        b_ref[1, :, lanes] = re * s + im * c
        c, s = rotate(tab_ref[0, :, lanes], tab_ref[1, :, lanes], dc, ds)
        for i in range(n):
            re = b_ref[0, i : i + 1, lanes]
            im = b_ref[1, i : i + 1, lanes]
            rc = re * c
            js = im * s
            jc = im * c
            rs = re * s
            at = i * LAGS
            y_ref[at : at + LAGS, lanes] = jnp.concatenate([rc - js, rc + js], axis=0).astype(BF16)
            y_ref[cols + at : cols + at + LAGS, lanes] = jnp.concatenate(
                [jc + rs, jc - rs], axis=0
            ).astype(BF16)

    g = jnp.concatenate([g_ref[0, 0], g_ref[1, 0]], axis=0)
    acc_ref[...] += dot_t(y_ref[...], g)

    @pl.when(step == steps - 1)
    def _():
        part = tsub // freqs
        acc = acc_ref[...]
        swap = pltpu.roll(acc, LANES - tsub, 1)
        corr_real = acc[:cols] + swap[cols:]
        corr_imag = acc[cols:] - swap[:cols]
        lane = lax.broadcasted_iota(jnp.int32, (1, LANES), 1)

        def pack(dest):
            real, imag = corr_real, pltpu.roll(corr_imag, part, 1)
            for d in range(1, freqs):
                here = dest == d
                real = jnp.where(here, pltpu.roll(corr_real, LANES - d * part, 1), real)
                moved = corr_imag if d == 1 else pltpu.roll(corr_imag, LANES - (d - 1) * part, 1)
                imag = jnp.where(here, moved, imag)
            return jnp.where(lane < part, real, jnp.where(lane < 2 * part, imag, 0.0))

        keep_ref[...] = pack(freq)
        for k in range(1, freqs):
            send_ref[k - 1] = pack(lax.rem(freq + k, freqs))


def fine_final_kernel(keep_ref, norm_ref, *rest, freqs, n, part, line):
    recv_refs = rest[: 2 * (freqs - 1)]
    out_refs = rest[2 * (freqs - 1) :]
    x = keep_ref[...]
    norm = norm_ref[line : line + 1, :]
    for k in range(freqs - 1):
        x = x + recv_refs[2 * k][0]
        norm = norm + recv_refs[2 * k + 1][0, line : line + 1, :]
    e = x * x
    e = e + pltpu.roll(e, LANES - part, 1)
    for i in range(n):
        top = jnp.max(e[i * LAGS : (i + 1) * LAGS], axis=0, keepdims=True)
        out_refs[i // CAP][i % CAP : i % CAP + 1, :] = top / norm


def params(mib=40, **kw):
    return pltpu.CompilerParams(vmem_limit_bytes=mib * 1024 * 1024, **kw)


SMEM = pl.BlockSpec(memory_space=pltpu.SMEM)


def coarse_section(info, weight, templates, blocks, banks, freqs, period):
    segs = blocks[0].shape[0]
    rows, bins = templates.shape[1], templates.shape[2]
    total = banks * segs
    cols = total * LAGS
    kc = min(2048, bins)
    steps = bins // kc
    part = rows // freqs
    kernel = functools.partial(
        coarse_kernel, blocks=len(blocks), segs=segs, banks=banks, freqs=freqs, steps=steps, kc=kc, period=period
    )
    return pl.pallas_call(
        kernel,
        grid=(steps,),
        in_specs=[
            SMEM,
            pl.BlockSpec((1, kc), lambda i: (0, i)),
            pl.BlockSpec((2, rows, kc), lambda i: (0, 0, i)),
        ]
        + [pl.BlockSpec((segs, 2, kc), lambda i: (0, 0, i)) for _ in blocks],
        out_specs=[
            pl.BlockSpec((part, 2 * cols), lambda i: (0, 0)),
            pl.BlockSpec((freqs - 1, part, 2 * cols), lambda i: (0, 0, 0)),
        ],
        out_shape=[
            jax.ShapeDtypeStruct((part, 2 * cols), F32),
            jax.ShapeDtypeStruct((freqs - 1, part, 2 * cols), F32),
        ],
        scratch_shapes=[
            pltpu.VMEM((banks, 2 * segs, kc), F32),
            pltpu.VMEM((2, total, kc), F32),
            pltpu.VMEM((2 * cols, 2 * kc), BF16),
            pltpu.VMEM((rows, 2 * cols), F32),
            pltpu.VMEM((4, PAIRS, kc), F32),
            pltpu.VMEM((2, PAIRS, kc), F32),
        ],
        compiler_params=params(dimension_semantics=("arbitrary",)),
        cost_estimate=pl.CostEstimate(
            flops=8 * rows * bins * cols, bytes_accessed=4 * rows * bins, transcendentals=0
        ),
        name="coarse",
    )(info, weight, templates, *blocks)


def fine_section(info, weight, mult, templates, blocks, freqs, period):
    bins = templates.shape[3]
    tsub = templates.shape[2]
    n = CAP * len(blocks)
    cols = n * LAGS
    kc = min(4096, bins)
    steps = bins // kc
    kernel = functools.partial(
        fine_kernel, blocks=len(blocks), freqs=freqs, steps=steps, kc=kc, period=period
    )
    return pl.pallas_call(
        kernel,
        grid=(steps,),
        in_specs=[
            SMEM,
            pl.BlockSpec((1, kc), lambda i: (0, i)),
            pl.BlockSpec((n, LANES), lambda i: (0, 0)),
            pl.BlockSpec((2, 1, tsub, kc), lambda i: (0, 0, 0, i)),
        ]
        + [pl.BlockSpec((CAP, 2, kc), lambda i: (0, 0, i)) for _ in blocks],
        out_specs=[
            pl.BlockSpec((cols, LANES), lambda i: (0, 0)),
            pl.BlockSpec((freqs - 1, cols, LANES), lambda i: (0, 0, 0)),
        ],
        out_shape=[
            jax.ShapeDtypeStruct((cols, LANES), F32),
            jax.ShapeDtypeStruct((freqs - 1, cols, LANES), F32),
        ],
        scratch_shapes=[
            pltpu.VMEM((2, n, kc), F32),
            pltpu.VMEM((2, n, kc), F32),
            pltpu.VMEM((2 * cols, kc), BF16),
            pltpu.VMEM((2 * cols, LANES), F32),
            pltpu.VMEM((2, PAIRS, kc), F32),
            pltpu.VMEM((2, n, kc), F32),
        ],
        compiler_params=params(dimension_semantics=("arbitrary",)),
        cost_estimate=pl.CostEstimate(
            flops=8 * tsub * bins * cols, bytes_accessed=4 * tsub * bins, transcendentals=0
        ),
        name="fine",
    )(info, weight, mult, templates, *blocks)


def after(value, *others):
    return lax.optimization_barrier((value, *others))[0]


def shift_permute(value, axis, count, by):
    return lax.ppermute(value, axis, [(i, (i + by) % count) for i in range(count)])


def norm_section(info, coarse_weight, fine_weight, coarse_templates, fine_templates, freqs):
    rows, bins = coarse_templates.shape[1:]
    tsub, fine_bins = fine_templates.shape[2:]
    part = rows // freqs
    lines = -(-(max(part // LANES, 1) + 1) // 8) * 8
    steps = 8
    kc, kf = bins // steps, fine_bins // steps
    return pl.pallas_call(
        functools.partial(norm_kernel, freqs=freqs, steps=steps),
        grid=(steps,),
        in_specs=[
            SMEM,
            pl.BlockSpec((1, kc), lambda i: (0, i)),
            pl.BlockSpec((1, kf), lambda i: (0, i)),
            pl.BlockSpec((2, rows, kc), lambda i: (0, 0, i)),
            pl.BlockSpec((2, 1, tsub, kf), lambda i: (0, 0, 0, i)),
        ],
        out_specs=[
            pl.BlockSpec((lines, LANES), lambda i: (0, 0)),
            pl.BlockSpec((freqs - 1, lines, LANES), lambda i: (0, 0, 0)),
        ],
        out_shape=[
            jax.ShapeDtypeStruct((lines, LANES), F32),
            jax.ShapeDtypeStruct((freqs - 1, lines, LANES), F32),
        ],
        scratch_shapes=[pltpu.VMEM((rows, LANES), F32), pltpu.VMEM((tsub, LANES), F32)],
        compiler_params=params(16, dimension_semantics=("arbitrary",)),
        cost_estimate=pl.CostEstimate(
            flops=8 * 10**9, bytes_accessed=4 * (rows * bins + tsub * fine_bins), transcendentals=0
        ),
        name="norms",
    )(info, coarse_weight, fine_weight, coarse_templates, fine_templates)


def body(
    coarse_spectra,
    fine_spectra,
    coarse_templates,
    fine_templates,
    coarse_weight,
    fine_weight,
    triggers,
    offsets,
):
    banks = lax.axis_size("bank")
    freqs = lax.axis_size("freq")
    bank = lax.axis_index("bank")
    freq = lax.axis_index("freq")
    segs = fine_spectra.shape[0]
    coarse_bins = coarse_spectra.shape[2]
    fine_bins = fine_spectra.shape[2]
    top = triggers.shape[1]
    tsub = fine_templates.shape[2]
    part = tsub // freqs
    coarse_period = 4 * coarse_bins * freqs
    fine_period = 4 * fine_bins * freqs
    zero = jnp.zeros((), jnp.int32)
    coarse_info = jnp.stack([freq * coarse_bins, bank, freq, zero]).astype(jnp.int32)
    fine_info = jnp.stack([freq * fine_bins, bank, freq, zero]).astype(jnp.int32)
    coarse_weight = coarse_weight.reshape(1, -1)
    fine_weight = fine_weight.reshape(1, -1)

    coarse_blocks = [coarse_spectra] + [
        shift_permute(coarse_spectra, "bank", banks, k) for k in range(1, banks)
    ]

    *picked, mult = pl.pallas_call(
        functools.partial(pick_kernel, banks=banks, segs=segs, top=top),
        in_specs=[SMEM, SMEM, SMEM, pl.BlockSpec(memory_space=pltpu.HBM)],
        out_shape=[jax.ShapeDtypeStruct((CAP, 2, fine_bins), BF16) for _ in range(banks)]
        + [jax.ShapeDtypeStruct((banks * CAP, LANES), jnp.int32)],
        scratch_shapes=[pltpu.SemaphoreType.DMA((banks * CAP,))],
        compiler_params=params(8),
        name="pick",
    )(fine_info, triggers, offsets, fine_spectra)
    order = sorted(range(banks), key=lambda k: min(k, banks - k))
    fine_blocks = {k: picked[k] if k == 0 else shift_permute(picked[k], "bank", banks, k) for k in order}

    norms, send_norms = norm_section(
        after(coarse_info, mult), coarse_weight, fine_weight, coarse_templates, fine_templates, freqs
    )
    line = max(coarse_templates.shape[1] // freqs // LANES, 1)
    recv_norms = [shift_permute(send_norms[k - 1 : k], "freq", freqs, k) for k in range(1, freqs)]

    keep, send = coarse_section(
        after(coarse_info, norms), coarse_weight, coarse_templates, coarse_blocks, banks, freqs, coarse_period
    )
    coarse_received = []
    for k in range(1, freqs):
        coarse_received += [shift_permute(send[k - 1 : k], "freq", freqs, k), recv_norms[k - 1]]
    last = coarse_keep = keep
    back = {}
    for members in (order[:-1], order[-1:]):
        keep, send = fine_section(
            after(fine_info, last),
            fine_weight,
            jnp.concatenate([mult[CAP * k : CAP * (k + 1)] for k in members], axis=0),
            fine_templates,
            [fine_blocks[k] for k in members],
            freqs,
            fine_period,
        )
        last = keep
        received = []
        for k in range(1, freqs):
            received += [shift_permute(send[k - 1 : k], "freq", freqs, k), recv_norms[k - 1]]
        results = pl.pallas_call(
            functools.partial(fine_final_kernel, freqs=freqs, n=CAP * len(members), part=part, line=line),
            out_shape=[jax.ShapeDtypeStruct((CAP, LANES), F32) for _ in members],
            compiler_params=params(8),
            name="fine_final",
        )(keep, norms, *received)
        for k, result in zip(members, results):
            back[k] = result if k == 0 else shift_permute(result, "bank", banks, banks - k)
    coarse_snr = pl.pallas_call(
        functools.partial(coarse_final_kernel, freqs=freqs, total=banks * segs),
        out_shape=jax.ShapeDtypeStruct((banks * segs, coarse_keep.shape[0]), F32),
        compiler_params=params(16),
        name="coarse_final",
    )(coarse_keep, after(norms, last), *coarse_received).T

    fine_snr = pl.pallas_call(
        functools.partial(place_kernel, banks=banks, segs=segs, top=top),
        in_specs=[SMEM, SMEM] + [pl.BlockSpec(memory_space=pltpu.VMEM) for _ in range(banks)],
        out_shape=jax.ShapeDtypeStruct((segs, top, part), F32),
        scratch_shapes=[pltpu.VMEM((banks * CAP, LANES), F32)],
        compiler_params=params(8),
        name="place",
    )(fine_info, triggers, *[back[k] for k in range(banks)])
    return (coarse_snr, fine_snr)


def solution(mesh):
    return jax.shard_map(
        body,
        mesh=mesh,
        in_specs=(
            P(("groups", "seg", "bank"), None, "freq"),
            P(("groups", "seg", "bank"), None, "freq"),
            P(None, "bank", "freq"),
            P(None, "bank", None, "freq"),
            P(("groups", "freq")),
            P(("groups", "freq")),
            P(("groups", "seg"), None),
            P(("groups", "seg"), None),
        ),
        out_specs=(
            P(("bank", "freq"), ("groups", "seg")),
            P(("groups", "seg", "bank"), None, "freq"),
        ),
        check_vma=False,
    )
```

```python
import functools
import math

import jax
import jax.numpy as jnp
from jax import lax
from jax.experimental import pallas as pl
from jax.experimental.pallas import tpu as pltpu
from jax.sharding import PartitionSpec as P


CAP = 2
LAGS = 16
PAIRS = LAGS // 2
CSTRIDE = 2047
LANES = 128
F32 = jnp.float32
BF16 = jnp.bfloat16


def sincos(counts, period):
    half = period // 2
    signed = ((counts + half) & (period - 1)) - half
    x = signed.astype(F32) * (1.0 / period)
    u = x * x
    p = math.pi
    s = -(p**11) / 39916800.0
    for a in (p**9 / 362880.0, -(p**7) / 5040.0, p**5 / 120.0, -(p**3) / 6.0, p):
        s = s * u + a
    s = s * x
    c = p**12 / 479001600.0
    for a in (-(p**10) / 3628800.0, p**8 / 40320.0, -(p**6) / 720.0, p**4 / 24.0, -(p**2) / 2.0, 1.0):
        c = c * u + a
    return 1.0 - 2.0 * s * s, 2.0 * s * c


def dot_t(a, b):
    return lax.dot_general(a, b, (((1,), (1,)), ((), ())), preferred_element_type=F32)


def rotate(c, s, dc, ds):
    return c * dc - s * ds, s * dc + c * ds


def norm_add(acc_ref, w, load, bins):
    rows = acc_ref.shape[0]
    chunk = min(rows, 64)
    for r in range(0, rows, chunk):
        n = acc_ref[r : r + chunk, :]
        for lo in range(0, bins, LANES):
            re = load(0, r, chunk, lo).astype(F32)
            im = load(1, r, chunk, lo).astype(F32)
            n = n + (re * re + im * im) * w[:, lo : lo + LANES]
        acc_ref[r : r + chunk, :] = n


def norm_row(n):
    if n.shape[0] < LANES:
        n = jnp.concatenate([n, jnp.zeros((LANES - n.shape[0], LANES), F32)], axis=0)
    return jnp.sum(n.T, axis=0, keepdims=True)


def coarse_kernel(
    info_ref, w_ref, h_ref, *rest, blocks, segs, banks, freqs, steps, kc, period
):
    spec_refs = rest[:blocks]
    keep_ref, send_ref = rest[blocks : blocks + 2]
    a_refs, b_refs, y_refs = (rest[blocks + i : blocks + i + 2] for i in (2, 4, 6))
    acc_ref, nacc_ref, tab_ref, ctr_ref = rest[blocks + 8 :]
    step = pl.program_id(0)
    base = info_ref[0]
    bank = info_ref[1]
    freq = info_ref[2]
    total = banks * segs
    cols = total * LAGS

    def gen(which, chunk):
        a_ref, b_ref, y_ref = a_refs[which], b_refs[which], y_refs[which]
        shift = pl.multiple_of(chunk * kc, kc)
        w = w_ref[:, pl.ds(shift, kc)]
        for k in range(blocks):
            source = lax.rem(bank - k + banks, banks)
            for i in range(segs):
                a_ref[source, 2 * i : 2 * i + 2, :] = spec_refs[k][i, :, pl.ds(shift, kc)].astype(F32) * w
        odd = 2 * lax.broadcasted_iota(jnp.int32, (PAIRS, LANES), 0) + 1
        dc, ds = sincos(shift * odd * CSTRIDE, period)
        ec, es = sincos(jnp.full((PAIRS, LANES), shift * (15 * CSTRIDE), jnp.int32), period)
        for lo in range(0, kc, LANES):
            lanes = slice(lo, lo + LANES)
            c, s = rotate(ctr_ref[0, :, lanes], ctr_ref[1, :, lanes], ec, es)
            for b in range(0, total, 4):
                re, im = (
                    jnp.concatenate(
                        [a_ref[(b + i) // segs, 2 * ((b + i) % segs) + c : 2 * ((b + i) % segs) + c + 1, lanes] for i in range(4)],
                        axis=0,
                    )
                    for c in range(2)
                )
                b_ref[0, b : b + 4, lanes] = re * c[:4] - im * s[:4]
                b_ref[1, b : b + 4, lanes] = re * s[:4] + im * c[:4]
            c, s = rotate(tab_ref[0, :, lanes], tab_ref[1, :, lanes], dc, ds)
            b_ref[2, :PAIRS, lanes] = c
            b_ref[3, :PAIRS, lanes] = s
            re = b_ref[0, :, lanes]
            im = b_ref[1, :, lanes]
            for m in range(PAIRS):
                cm = b_ref[2, m : m + 1, lanes]
                sm = b_ref[3, m : m + 1, lanes]
                rc = re * cm
                js = im * sm
                jc = im * cm
                rs = re * sm
                for sign, (yr, yi) in enumerate(((rc - js, jc + rs), (rc + js, jc - rs))):
                    at = (2 * m + sign) * total
                    yr = yr.astype(BF16)
                    yi = yi.astype(BF16)
                    y_ref[at : at + total, lo : lo + LANES] = yr
                    y_ref[at : at + total, kc + lo : kc + lo + LANES] = yi
                    y_ref[cols + at : cols + at + total, lo : lo + LANES] = yi
                    y_ref[cols + at : cols + at + total, kc + lo : kc + lo + LANES] = -yr

    @pl.when(step == 0)
    def _():
        ids = base + lax.broadcasted_iota(jnp.int32, (PAIRS, kc), 1)
        odd = 2 * lax.broadcasted_iota(jnp.int32, (PAIRS, kc), 0) + 1
        c, s = sincos(ids * odd * CSTRIDE, period)
        tab_ref[0] = c
        tab_ref[1] = s
        c, s = sincos(ids * (15 * CSTRIDE), period)
        ctr_ref[0] = c
        ctr_ref[1] = s
        acc_ref[...] = jnp.zeros_like(acc_ref)
        nacc_ref[...] = jnp.zeros_like(nacc_ref)
        gen(0, step)

    for half in range(2):
        lo = half * kc
        gen(1 - half, jnp.minimum(2 * step + half + 1, 2 * steps - 1))
        h = jnp.concatenate([h_ref[0, :, lo : lo + kc], h_ref[1, :, lo : lo + kc]], axis=1)
        acc_ref[...] += dot_t(h, y_refs[half][...])
    w = w_ref[:, pl.ds(pl.multiple_of(step * 2 * kc, 2 * kc), 2 * kc)]
    norm_add(nacc_ref, w, lambda c, r, n, lo: h_ref[c, r : r + n, lo : lo + LANES], 2 * kc)

    @pl.when(step == steps - 1)
    def _():
        part = acc_ref.shape[0] // freqs
        size = min(part, LANES)

        def lay(ref, dest):
            first = pl.multiple_of(dest * part, part)
            ref[:part, :] = acc_ref[pl.ds(first, part), :]
            for r in range(0, part, size):
                row = norm_row(nacc_ref[pl.ds(first + r, size), :])
                ref[part : part + 8, r : r + LANES] = jnp.broadcast_to(row, (8, LANES))

        lay(keep_ref, freq)
        for k in range(1, freqs):
            lay(send_ref.at[k - 1], lax.rem(freq + k, freqs))


def coarse_final_kernel(keep_ref, *rest, freqs, total):
    recv_refs = rest[: freqs - 1]
    out_ref = rest[freqs - 1]
    part = keep_ref.shape[0] - 8
    cols = total * LAGS
    corr = keep_ref[...]
    for ref in recv_refs:
        corr = corr + ref[0]
    norms = corr[part : part + 1]
    cr = corr[:part, :cols]
    ci = corr[:part, cols:]
    e = cr * cr + ci * ci
    width = cols
    while width > max(total, LANES):
        width //= 2
        e = jnp.maximum(e[:, :width], e[:, width:])
    while width > total:
        width //= 2
        e = jnp.maximum(e, pltpu.roll(e, LANES - width, 1))
    size = min(part, LANES)
    for r in range(0, part, size):
        rows = e[r : r + size]
        if size < LANES:
            rows = jnp.concatenate([rows, jnp.zeros((LANES - size, LANES), F32)], axis=0)
        out = rows.T[:total] / norms[:, r : r + LANES]
        out_ref[:, r : r + size] = out[:, :size]


def ranked_pairs(trig_ref, first, segs, top, target):
    taken = jnp.int32(0)
    found = [jnp.int32(0) for _ in range(CAP)]
    for p in range(segs * top):
        hit = (trig_ref[p % top, first + p // top] == target).astype(jnp.int32)
        for c in range(CAP):
            found[c] = jnp.where(jnp.logical_and(hit == 1, taken == c), p, found[c])
        taken = taken + hit
    return taken, found


def pick_kernel(info_ref, trig_ref, off_ref, spec_ref, *rest, banks, segs, top):
    out_refs = rest[:banks]
    mult_ref, sems = rest[banks:]
    bank = info_ref[1]
    copies = []
    for k in range(banks):
        k = (k + 1) % banks
        dest = lax.rem(bank + k, banks)
        _, found = ranked_pairs(trig_ref, bank * segs, segs, top, dest)
        for c in range(CAP):
            copy = pltpu.make_async_copy(
                spec_ref.at[found[c] // top], out_refs[k].at[c], sems.at[k * CAP + c]
            )
            copy.start()
            copies.append(copy)
    line = lax.broadcasted_iota(jnp.int32, mult_ref.shape, 0)
    mult = jnp.zeros(mult_ref.shape, jnp.int32)
    for k in range(banks):
        source = lax.rem(bank - k + banks, banks)
        _, found = ranked_pairs(trig_ref, source * segs, segs, top, bank)
        for c in range(CAP):
            offset = off_ref[lax.rem(found[c], top), source * segs + found[c] // top]
            mult = jnp.where(line == k * CAP + c, 2 * offset + (LAGS - 1), mult)
    mult_ref[...] = mult
    for copy in copies:
        copy.wait()


def place_kernel(info_ref, trig_ref, *rest, banks, segs, top):
    back_refs = rest[:banks]
    out_ref, all_ref = rest[banks:]
    bank = info_ref[1]
    part = out_ref.shape[2]
    for k in range(banks):
        all_ref[CAP * k : CAP * (k + 1), :] = back_refs[k][...]
    for p in range(segs * top):
        target = trig_ref[p % top, bank * segs + p // top]
        rank = jnp.int32(0)
        for q in range(p):
            rank = rank + (trig_ref[q % top, bank * segs + q // top] == target).astype(jnp.int32)
        at = lax.rem(target - bank + banks, banks) * CAP + jnp.minimum(rank, CAP - 1)
        out_ref[p // top, p % top : p % top + 1, :] = all_ref[pl.ds(at, 1), :][:, :part]


def fine_kernel(info_ref, w_ref, mult_ref, g_ref, *rest, blocks, freqs, steps, kc, period):
    slot_refs = rest[:blocks]
    keep_ref, send_ref = rest[blocks : blocks + 2]
    a_refs, b_refs, y_refs = (rest[blocks + i : blocks + i + 2] for i in (2, 4, 6))
    acc_ref, nacc_ref, tab_ref, ctr_ref = rest[blocks + 8 :]
    step = pl.program_id(0)
    base = info_ref[0]
    freq = info_ref[2]
    n = blocks * CAP
    cols = n * LAGS
    tsub = g_ref.shape[2]

    def gen(which, chunk):
        a_ref, b_ref, y_ref = a_refs[which], b_refs[which], y_refs[which]
        shift = pl.multiple_of(chunk * kc, kc)
        w = w_ref[:, pl.ds(shift, kc)]
        for k in range(blocks):
            for i in range(CAP):
                x = slot_refs[k][i, :, pl.ds(shift, kc)].astype(F32) * w
                a_ref[0, CAP * k + i : CAP * k + i + 1, :] = x[0:1]
                a_ref[1, CAP * k + i : CAP * k + i + 1, :] = x[1:2]
        odd = 2 * lax.broadcasted_iota(jnp.int32, (PAIRS, LANES), 0) + 1
        dc, ds = sincos(shift * odd, period)
        ec, es = sincos(shift * mult_ref[...], period)
        for lo in range(0, kc, LANES):
            lanes = slice(lo, lo + LANES)
            c, s = rotate(ctr_ref[0, :, lanes], ctr_ref[1, :, lanes], ec, es)
            re = a_ref[0, :, lanes]
            im = a_ref[1, :, lanes]
            b_ref[0, :, lanes] = re * c - im * s
            b_ref[1, :, lanes] = re * s + im * c
            c, s = rotate(tab_ref[0, :, lanes], tab_ref[1, :, lanes], dc, ds)
            for i in range(n):
                re = b_ref[0, i : i + 1, lanes]
                im = b_ref[1, i : i + 1, lanes]
                rc = re * c
                js = im * s
                jc = im * c
                rs = re * s
                at = i * LAGS
                y_ref[at : at + LAGS, lanes] = jnp.concatenate([rc - js, rc + js], axis=0).astype(BF16)
                y_ref[cols + at : cols + at + LAGS, lanes] = jnp.concatenate(
                    [jc + rs, jc - rs], axis=0
                ).astype(BF16)

    @pl.when(step == 0)
    def _():
        ids = base + lax.broadcasted_iota(jnp.int32, (PAIRS, kc), 1)
        odd = 2 * lax.broadcasted_iota(jnp.int32, (PAIRS, kc), 0) + 1
        c, s = sincos(ids * odd, period)
        tab_ref[0] = c
        tab_ref[1] = s
        ids = base + lax.broadcasted_iota(jnp.int32, (n, kc), 1)
        c, s = sincos(ids * mult_ref[:, 0:1], period)
        ctr_ref[0] = c
        ctr_ref[1] = s
        acc_ref[...] = jnp.zeros_like(acc_ref)
        nacc_ref[...] = jnp.zeros_like(nacc_ref)
        gen(0, step)

    for half in range(2):
        lo = half * kc
        gen(1 - half, jnp.minimum(2 * step + half + 1, 2 * steps - 1))
        g = jnp.concatenate([g_ref[0, 0, :, lo : lo + kc], g_ref[1, 0, :, lo : lo + kc]], axis=0)
        acc_ref[...] += dot_t(y_refs[half][...], g)
    w = w_ref[:, pl.ds(pl.multiple_of(step * 2 * kc, 2 * kc), 2 * kc)]
    norm_add(nacc_ref, w, lambda c, r, n, lo: g_ref[c, 0, r : r + n, lo : lo + LANES], 2 * kc)

    @pl.when(step == steps - 1)
    def _():
        part = tsub // freqs
        acc = acc_ref[...]
        swap = pltpu.roll(acc, LANES - tsub, 1)
        corr_real = acc[:cols] + swap[cols:]
        corr_imag = acc[cols:] - swap[:cols]
        lane = lax.broadcasted_iota(jnp.int32, (1, LANES), 1)
        norms = jnp.broadcast_to(norm_row(nacc_ref[...]), (8, LANES))

        def pack(dest):
            real, imag = corr_real, pltpu.roll(corr_imag, part, 1)
            for d in range(1, freqs):
                here = dest == d
                real = jnp.where(here, pltpu.roll(corr_real, LANES - d * part, 1), real)
                moved = corr_imag if d == 1 else pltpu.roll(corr_imag, LANES - (d - 1) * part, 1)
                imag = jnp.where(here, moved, imag)
            row = norms
            for d in range(1, freqs):
                row = jnp.where(dest == d, pltpu.roll(norms, LANES - d * part, 1), row)
            return jnp.concatenate(
                [jnp.where(lane < part, real, jnp.where(lane < 2 * part, imag, 0.0)), row], axis=0
            )

        keep_ref[...] = pack(freq)
        for k in range(1, freqs):
            send_ref[k - 1] = pack(lax.rem(freq + k, freqs))


def fine_final_kernel(keep_ref, *rest, freqs, n, part):
    recv_refs = rest[: freqs - 1]
    out_refs = rest[freqs - 1 :]
    x = keep_ref[...]
    for ref in recv_refs:
        x = x + ref[0]
    norm = x[n * LAGS : n * LAGS + 1]
    e = x[: n * LAGS]
    e = e * e
    e = e + pltpu.roll(e, LANES - part, 1)
    for i in range(n):
        top = jnp.max(e[i * LAGS : (i + 1) * LAGS], axis=0, keepdims=True)
        out_refs[i // CAP][i % CAP : i % CAP + 1, :] = top / norm


def params(mib=50, **kw):
    return pltpu.CompilerParams(vmem_limit_bytes=mib * 1024 * 1024, **kw)


SMEM = pl.BlockSpec(memory_space=pltpu.SMEM)
VMEM = pl.BlockSpec(memory_space=pltpu.VMEM)


def coarse_section(info, weight, templates, blocks, banks, freqs, period):
    segs = blocks[0].shape[0]
    rows, bins = templates.shape[1], templates.shape[2]
    total = banks * segs
    cols = total * LAGS
    kc = min(1024, bins // 2)
    steps = bins // (2 * kc)
    part = rows // freqs
    kernel = functools.partial(
        coarse_kernel, blocks=len(blocks), segs=segs, banks=banks, freqs=freqs, steps=steps, kc=kc, period=period
    )
    return pl.pallas_call(
        kernel,
        grid=(steps,),
        in_specs=[
            SMEM,
            VMEM,
            pl.BlockSpec((2, rows, 2 * kc), lambda i: (0, 0, i)),
        ]
        + [VMEM for _ in blocks],
        out_specs=[
            pl.BlockSpec((part + 8, 2 * cols), lambda i: (0, 0)),
            pl.BlockSpec((freqs - 1, part + 8, 2 * cols), lambda i: (0, 0, 0)),
        ],
        out_shape=[
            jax.ShapeDtypeStruct((part + 8, 2 * cols), F32),
            jax.ShapeDtypeStruct((freqs - 1, part + 8, 2 * cols), F32),
        ],
        scratch_shapes=[
            *[pltpu.VMEM((banks, 2 * segs, kc), F32) for _ in range(2)],
            *[pltpu.VMEM((4, total, kc), F32) for _ in range(2)],
            *[pltpu.VMEM((2 * cols, 2 * kc), BF16) for _ in range(2)],
            pltpu.VMEM((rows, 2 * cols), F32),
            pltpu.VMEM((rows, LANES), F32),
            pltpu.VMEM((2, PAIRS, kc), F32),
            pltpu.VMEM((2, PAIRS, kc), F32),
        ],
        compiler_params=params(dimension_semantics=("arbitrary",)),
        cost_estimate=pl.CostEstimate(
            flops=8 * rows * bins * cols, bytes_accessed=4 * rows * bins, transcendentals=0
        ),
        name="coarse",
    )(info, weight, templates, *blocks)


def fine_section(info, weight, mult, templates, blocks, freqs, period):
    bins = templates.shape[3]
    tsub = templates.shape[2]
    n = CAP * len(blocks)
    cols = n * LAGS
    kc = min(2048, bins // 2)
    steps = bins // (2 * kc)
    kernel = functools.partial(
        fine_kernel, blocks=len(blocks), freqs=freqs, steps=steps, kc=kc, period=period
    )
    return pl.pallas_call(
        kernel,
        grid=(steps,),
        in_specs=[
            SMEM,
            VMEM,
            VMEM,
            pl.BlockSpec((2, 1, tsub, 2 * kc), lambda i: (0, 0, 0, i)),
        ]
        + [VMEM for _ in blocks],
        out_specs=[
            pl.BlockSpec((cols + 8, LANES), lambda i: (0, 0)),
            pl.BlockSpec((freqs - 1, cols + 8, LANES), lambda i: (0, 0, 0)),
        ],
        out_shape=[
            jax.ShapeDtypeStruct((cols + 8, LANES), F32),
            jax.ShapeDtypeStruct((freqs - 1, cols + 8, LANES), F32),
        ],
        scratch_shapes=[
            *[pltpu.VMEM((2, n, kc), F32) for _ in range(4)],
            *[pltpu.VMEM((2 * cols, kc), BF16) for _ in range(2)],
            pltpu.VMEM((2 * cols, LANES), F32),
            pltpu.VMEM((tsub, LANES), F32),
            pltpu.VMEM((2, PAIRS, kc), F32),
            pltpu.VMEM((2, n, kc), F32),
        ],
        compiler_params=params(dimension_semantics=("arbitrary",)),
        cost_estimate=pl.CostEstimate(
            flops=8 * tsub * bins * cols, bytes_accessed=4 * tsub * bins, transcendentals=0
        ),
        name="fine",
    )(info, weight, mult, templates, *blocks)


def after(value, *others):
    return lax.optimization_barrier((value, *others))[0]


def shift_permute(value, axis, count, by):
    return lax.ppermute(value, axis, [(i, (i + by) % count) for i in range(count)])


def body(
    coarse_spectra,
    fine_spectra,
    coarse_templates,
    fine_templates,
    coarse_weight,
    fine_weight,
    triggers,
    offsets,
):
    banks = lax.axis_size("bank")
    freqs = lax.axis_size("freq")
    bank = lax.axis_index("bank")
    freq = lax.axis_index("freq")
    segs = fine_spectra.shape[0]
    coarse_bins = coarse_spectra.shape[2]
    fine_bins = fine_spectra.shape[2]
    top = triggers.shape[1]
    tsub = fine_templates.shape[2]
    part = tsub // freqs
    coarse_period = 4 * coarse_bins * freqs
    fine_period = 4 * fine_bins * freqs
    zero = jnp.zeros((), jnp.int32)
    coarse_info = jnp.stack([freq * coarse_bins, bank, freq, zero]).astype(jnp.int32)
    fine_info = jnp.stack([freq * fine_bins, bank, freq, zero]).astype(jnp.int32)
    coarse_weight = coarse_weight.reshape(1, -1)
    fine_weight = fine_weight.reshape(1, -1)

    coarse_blocks = [coarse_spectra] + [
        shift_permute(coarse_spectra, "bank", banks, k) for k in range(1, banks)
    ]

    *picked, mult = pl.pallas_call(
        functools.partial(pick_kernel, banks=banks, segs=segs, top=top),
        in_specs=[SMEM, SMEM, SMEM, pl.BlockSpec(memory_space=pltpu.HBM)],
        out_shape=[jax.ShapeDtypeStruct((CAP, 2, fine_bins), BF16) for _ in range(banks)]
        + [jax.ShapeDtypeStruct((banks * CAP, LANES), jnp.int32)],
        scratch_shapes=[pltpu.SemaphoreType.DMA((banks * CAP,))],
        compiler_params=params(),
        name="pick",
    )(fine_info, triggers.T, offsets.T, fine_spectra)
    order = sorted(range(banks), key=lambda k: min(k, banks - k))
    fine_blocks = {}
    for k in order:
        fine_blocks[k] = picked[k] if k == 0 else shift_permute(picked[k], "bank", banks, k)

    def exchange(send):
        return [shift_permute(send[k - 1 : k], "freq", freqs, k) for k in range(1, freqs)]

    keep, send = coarse_section(
        coarse_info, coarse_weight, coarse_templates, coarse_blocks, banks, freqs, coarse_period
    )
    coarse_keep, coarse_received = keep, exchange(send)
    done = [keep]
    back = {}
    for members in (order[:-1], order[-1:]):
        keep, send = fine_section(
            after(fine_info, *done),
            fine_weight,
            jnp.concatenate([mult[CAP * k : CAP * (k + 1)] for k in members], axis=0),
            fine_templates,
            [fine_blocks[k] for k in members],
            freqs,
            fine_period,
        )
        received = exchange(send)
        done = pl.pallas_call(
            functools.partial(fine_final_kernel, freqs=freqs, n=CAP * len(members), part=part),
            out_shape=[jax.ShapeDtypeStruct((CAP, LANES), F32) for _ in members],
            compiler_params=params(8),
            name="fine_final",
        )(keep, *received)
        for k, result in zip(members, done):
            back[k] = result if k == 0 else shift_permute(result, "bank", banks, banks - k)
    coarse_snr = pl.pallas_call(
        functools.partial(coarse_final_kernel, freqs=freqs, total=banks * segs),
        out_shape=jax.ShapeDtypeStruct((banks * segs, coarse_keep.shape[0] - 8), F32),
        compiler_params=params(16),
        name="coarse_final",
    )(after(coarse_keep, keep), *coarse_received).T
    fine_snr = pl.pallas_call(
        functools.partial(place_kernel, banks=banks, segs=segs, top=top),
        in_specs=[SMEM, SMEM] + [pl.BlockSpec(memory_space=pltpu.VMEM) for _ in range(banks)],
        out_shape=jax.ShapeDtypeStruct((segs, top, part), F32),
        scratch_shapes=[pltpu.VMEM((banks * CAP, LANES), F32)],
        compiler_params=params(8),
        name="place",
    )(fine_info, triggers.T, *[back[k] for k in range(banks)])
    return (coarse_snr, fine_snr)


def solution(mesh):
    return sharded(mesh)


def sharded(mesh):
    return jax.shard_map(
        body,
        mesh=mesh,
        in_specs=(
            P(("groups", "seg", "bank"), None, "freq"),
            P(("groups", "seg", "bank"), None, "freq"),
            P(None, "bank", "freq"),
            P(None, "bank", None, "freq"),
            P(("groups", "freq")),
            P(("groups", "freq")),
            P(("groups", "seg"), None),
            P(("groups", "seg"), None),
        ),
        out_specs=(
            P(("bank", "freq"), ("groups", "seg")),
            P(("groups", "seg", "bank"), None, "freq"),
        ),
        check_vma=False,
    )
```

```python
import functools
import math

import jax
import jax.numpy as jnp
from jax import lax
from jax.experimental import pallas as pl
from jax.experimental.pallas import tpu as pltpu
from jax.sharding import PartitionSpec as P


CAP = 2
LAGS = 16
PAIRS = LAGS // 2
CSTRIDE = 2047
LANES = 128
F32 = jnp.float32
BF16 = jnp.bfloat16


def sincos(counts, period):
    half = period // 2
    signed = ((counts + half) & (period - 1)) - half
    x = signed.astype(F32) * (1.0 / period)
    u = x * x
    p = math.pi
    s = -(p**11) / 39916800.0
    for a in (p**9 / 362880.0, -(p**7) / 5040.0, p**5 / 120.0, -(p**3) / 6.0, p):
        s = s * u + a
    s = s * x
    c = p**12 / 479001600.0
    for a in (-(p**10) / 3628800.0, p**8 / 40320.0, -(p**6) / 720.0, p**4 / 24.0, -(p**2) / 2.0, 1.0):
        c = c * u + a
    return 1.0 - 2.0 * s * s, 2.0 * s * c


def dot_t(a, b):
    return lax.dot_general(a, b, (((1,), (1,)), ((), ())), preferred_element_type=F32)


def rotate(c, s, dc, ds):
    return c * dc - s * ds, s * dc + c * ds


def norm_add(acc_ref, w, load, bins):
    rows = acc_ref.shape[0]
    chunk = min(rows, 64)
    for r in range(0, rows, chunk):
        n = acc_ref[r : r + chunk, :]
        for lo in range(0, bins, LANES):
            re = load(0, r, chunk, lo).astype(F32)
            im = load(1, r, chunk, lo).astype(F32)
            n = n + (re * re + im * im) * w[:, lo : lo + LANES]
        acc_ref[r : r + chunk, :] = n


def norm_row(n):
    if n.shape[0] < LANES:
        n = jnp.concatenate([n, jnp.zeros((LANES - n.shape[0], LANES), F32)], axis=0)
    return jnp.sum(n.T, axis=0, keepdims=True)


def coarse_kernel(
    info_ref, w_ref, h_ref, *rest, blocks, segs, banks, freqs, chunks, kc, period
):
    spec_refs = rest[:blocks]
    keep_ref, send_ref = rest[blocks : blocks + 2]
    a_refs, b_refs, y_refs = (rest[blocks + i : blocks + i + 2] for i in (2, 4, 6))
    acc_ref, nacc_ref, tab_ref, ctr_ref, held_ref, sems = rest[blocks + 8 :]
    base = info_ref[0]
    bank = info_ref[1]
    freq = info_ref[2]
    total = banks * segs
    cols = total * LAGS

    def fetch(chunk):
        at = pl.ds(pl.multiple_of(chunk * kc, kc), kc)
        return pltpu.make_async_copy(h_ref.at[:, :, at], held_ref.at[chunk], sems.at[chunk])

    for chunk in range(chunks):
        fetch(chunk).start()

    def gen(which, chunk):
        a_ref, b_ref, y_ref = a_refs[which], b_refs[which], y_refs[which]
        shift = pl.multiple_of(chunk * kc, kc)
        w = w_ref[:, pl.ds(shift, kc)]
        for k in range(blocks):
            source = lax.rem(bank - k + banks, banks)
            for i in range(segs):
                a_ref[source, 2 * i : 2 * i + 2, :] = spec_refs[k][i, :, pl.ds(shift, kc)].astype(F32) * w
        odd = 2 * lax.broadcasted_iota(jnp.int32, (PAIRS, LANES), 0) + 1
        dc, ds = sincos(shift * odd * CSTRIDE, period)
        ec, es = sincos(jnp.full((PAIRS, LANES), shift * (15 * CSTRIDE), jnp.int32), period)
        for lo in range(0, kc, LANES):
            lanes = slice(lo, lo + LANES)
            c, s = rotate(ctr_ref[0, :, lanes], ctr_ref[1, :, lanes], ec, es)
            for b in range(0, total, 4):
                re, im = (
                    jnp.concatenate(
                        [a_ref[(b + i) // segs, 2 * ((b + i) % segs) + c : 2 * ((b + i) % segs) + c + 1, lanes] for i in range(4)],
                        axis=0,
                    )
                    for c in range(2)
                )
                b_ref[0, b : b + 4, lanes] = re * c[:4] - im * s[:4]
                b_ref[1, b : b + 4, lanes] = re * s[:4] + im * c[:4]
            c, s = rotate(tab_ref[0, :, lanes], tab_ref[1, :, lanes], dc, ds)
            b_ref[2, :PAIRS, lanes] = c
            b_ref[3, :PAIRS, lanes] = s
            re = b_ref[0, :, lanes]
            im = b_ref[1, :, lanes]
            for m in range(PAIRS):
                cm = b_ref[2, m : m + 1, lanes]
                sm = b_ref[3, m : m + 1, lanes]
                rc = re * cm
                js = im * sm
                jc = im * cm
                rs = re * sm
                for sign, (yr, yi) in enumerate(((rc - js, jc + rs), (rc + js, jc - rs))):
                    at = (2 * m + sign) * total
                    yr = yr.astype(BF16)
                    yi = yi.astype(BF16)
                    y_ref[at : at + total, lo : lo + LANES] = yr
                    y_ref[at : at + total, kc + lo : kc + lo + LANES] = yi
                    y_ref[cols + at : cols + at + total, lo : lo + LANES] = yi
                    y_ref[cols + at : cols + at + total, kc + lo : kc + lo + LANES] = -yr

    ids = base + lax.broadcasted_iota(jnp.int32, (PAIRS, kc), 1)
    odd = 2 * lax.broadcasted_iota(jnp.int32, (PAIRS, kc), 0) + 1
    c, s = sincos(ids * odd * CSTRIDE, period)
    tab_ref[0] = c
    tab_ref[1] = s
    c, s = sincos(ids * (15 * CSTRIDE), period)
    ctr_ref[0] = c
    ctr_ref[1] = s
    acc_ref[...] = jnp.zeros_like(acc_ref)
    nacc_ref[...] = jnp.zeros_like(nacc_ref)
    gen(0, jnp.int32(0))

    def pair(turn, carry):
        fetch(2 * turn).wait()
        fetch(2 * turn + 1).wait()
        for half in range(2):
            chunk = 2 * turn + half
            gen(1 - half, jnp.minimum(chunk + 1, chunks - 1))
            w = w_ref[:, pl.ds(pl.multiple_of(chunk * kc, kc), kc)]
            norm_add(nacc_ref, w, lambda c, r, n, at: held_ref[chunk, c, r : r + n, at : at + LANES], kc)
            h = jnp.concatenate([held_ref[chunk, 0], held_ref[chunk, 1]], axis=1)
            acc_ref[...] += dot_t(h, y_refs[half][...])
        return carry

    lax.fori_loop(0, chunks // 2, pair, 0)
    part = acc_ref.shape[0] // freqs
    size = min(part, LANES)

    def lay(ref, dest):
        first = pl.multiple_of(dest * part, part)
        ref[:part, :] = acc_ref[pl.ds(first, part), :]
        for r in range(0, part, size):
            row = norm_row(nacc_ref[pl.ds(first + r, size), :])
            ref[part : part + 8, r : r + LANES] = jnp.broadcast_to(row, (8, LANES))

    lay(keep_ref, freq)
    for k in range(1, freqs):
        lay(send_ref.at[k - 1], lax.rem(freq + k, freqs))


def coarse_final_kernel(keep_ref, *rest, freqs, total):
    recv_refs = rest[: freqs - 1]
    out_ref = rest[freqs - 1]
    part = keep_ref.shape[0] - 8
    cols = total * LAGS
    corr = keep_ref[...]
    for ref in recv_refs:
        corr = corr + ref[0]
    norms = corr[part : part + 1]
    cr = corr[:part, :cols]
    ci = corr[:part, cols:]
    e = cr * cr + ci * ci
    width = cols
    while width > max(total, LANES):
        width //= 2
        e = jnp.maximum(e[:, :width], e[:, width:])
    while width > total:
        width //= 2
        e = jnp.maximum(e, pltpu.roll(e, LANES - width, 1))
    size = min(part, LANES)
    for r in range(0, part, size):
        rows = e[r : r + size]
        if size < LANES:
            rows = jnp.concatenate([rows, jnp.zeros((LANES - size, LANES), F32)], axis=0)
        out = rows.T[:total] / norms[:, r : r + LANES]
        out_ref[:, r : r + size] = out[:, :size]


def ranked_pairs(trig_ref, first, segs, top, target):
    taken = jnp.int32(0)
    found = [jnp.int32(0) for _ in range(CAP)]
    for p in range(segs * top):
        hit = (trig_ref[p % top, first + p // top] == target).astype(jnp.int32)
        for c in range(CAP):
            found[c] = jnp.where(jnp.logical_and(hit == 1, taken == c), p, found[c])
        taken = taken + hit
    return taken, found


def pick_kernel(info_ref, trig_ref, off_ref, spec_ref, *rest, banks, segs, top):
    out_refs = rest[:banks]
    mult_ref, sems = rest[banks:]
    bank = info_ref[1]
    copies = []
    for k in range(banks):
        k = (k + 1) % banks
        dest = lax.rem(bank + k, banks)
        _, found = ranked_pairs(trig_ref, bank * segs, segs, top, dest)
        for c in range(CAP):
            copy = pltpu.make_async_copy(
                spec_ref.at[found[c] // top], out_refs[k].at[c], sems.at[k * CAP + c]
            )
            copy.start()
            copies.append(copy)
    line = lax.broadcasted_iota(jnp.int32, mult_ref.shape, 0)
    mult = jnp.zeros(mult_ref.shape, jnp.int32)
    for k in range(banks):
        source = lax.rem(bank - k + banks, banks)
        _, found = ranked_pairs(trig_ref, source * segs, segs, top, bank)
        for c in range(CAP):
            offset = off_ref[lax.rem(found[c], top), source * segs + found[c] // top]
            mult = jnp.where(line == k * CAP + c, 2 * offset + (LAGS - 1), mult)
    mult_ref[...] = mult
    for copy in copies:
        copy.wait()


def place_kernel(info_ref, trig_ref, *rest, banks, segs, top):
    back_refs = rest[:banks]
    out_ref, all_ref = rest[banks:]
    bank = info_ref[1]
    part = out_ref.shape[2]
    for k in range(banks):
        all_ref[CAP * k : CAP * (k + 1), :] = back_refs[k][...]
    for p in range(segs * top):
        target = trig_ref[p % top, bank * segs + p // top]
        rank = jnp.int32(0)
        for q in range(p):
            rank = rank + (trig_ref[q % top, bank * segs + q // top] == target).astype(jnp.int32)
        at = lax.rem(target - bank + banks, banks) * CAP + jnp.minimum(rank, CAP - 1)
        out_ref[p // top, p % top : p % top + 1, :] = all_ref[pl.ds(at, 1), :][:, :part]


def fine_kernel(info_ref, w_ref, mult_ref, g_ref, *rest, blocks, freqs, chunks, kc, period):
    slot_refs = rest[:blocks]
    keep_ref, send_ref = rest[blocks : blocks + 2]
    a_refs, b_refs, y_refs = (rest[blocks + i : blocks + i + 2] for i in (2, 4, 6))
    acc_ref, nacc_ref, tab_ref, ctr_ref, held_ref, sems = rest[blocks + 8 :]
    base = info_ref[0]
    freq = info_ref[2]
    n = blocks * CAP
    cols = n * LAGS
    tsub = g_ref.shape[2]

    def fetch(chunk):
        at = pl.ds(pl.multiple_of(chunk * kc, kc), kc)
        return pltpu.make_async_copy(g_ref.at[:, 0, :, at], held_ref.at[chunk], sems.at[chunk])

    for chunk in range(chunks):
        fetch(chunk).start()

    def gen(which, chunk):
        a_ref, b_ref, y_ref = a_refs[which], b_refs[which], y_refs[which]
        shift = pl.multiple_of(chunk * kc, kc)
        w = w_ref[:, pl.ds(shift, kc)]
        for k in range(blocks):
            for i in range(CAP):
                x = slot_refs[k][i, :, pl.ds(shift, kc)].astype(F32) * w
                a_ref[0, CAP * k + i : CAP * k + i + 1, :] = x[0:1]
                a_ref[1, CAP * k + i : CAP * k + i + 1, :] = x[1:2]
        odd = 2 * lax.broadcasted_iota(jnp.int32, (PAIRS, LANES), 0) + 1
        dc, ds = sincos(shift * odd, period)
        ec, es = sincos(shift * mult_ref[...], period)
        for lo in range(0, kc, LANES):
            lanes = slice(lo, lo + LANES)
            c, s = rotate(ctr_ref[0, :, lanes], ctr_ref[1, :, lanes], ec, es)
            re = a_ref[0, :, lanes]
            im = a_ref[1, :, lanes]
            b_ref[0, :, lanes] = re * c - im * s
            b_ref[1, :, lanes] = re * s + im * c
            c, s = rotate(tab_ref[0, :, lanes], tab_ref[1, :, lanes], dc, ds)
            for i in range(n):
                re = b_ref[0, i : i + 1, lanes]
                im = b_ref[1, i : i + 1, lanes]
                rc = re * c
                js = im * s
                jc = im * c
                rs = re * s
                at = i * LAGS
                y_ref[at : at + LAGS, lanes] = jnp.concatenate([rc - js, rc + js], axis=0).astype(BF16)
                y_ref[cols + at : cols + at + LAGS, lanes] = jnp.concatenate(
                    [jc + rs, jc - rs], axis=0
                ).astype(BF16)

    ids = base + lax.broadcasted_iota(jnp.int32, (PAIRS, kc), 1)
    odd = 2 * lax.broadcasted_iota(jnp.int32, (PAIRS, kc), 0) + 1
    c, s = sincos(ids * odd, period)
    tab_ref[0] = c
    tab_ref[1] = s
    ids = base + lax.broadcasted_iota(jnp.int32, (n, kc), 1)
    c, s = sincos(ids * mult_ref[:, 0:1], period)
    ctr_ref[0] = c
    ctr_ref[1] = s
    acc_ref[...] = jnp.zeros_like(acc_ref)
    nacc_ref[...] = jnp.zeros_like(nacc_ref)
    gen(0, jnp.int32(0))

    def pair(turn, carry):
        fetch(2 * turn).wait()
        fetch(2 * turn + 1).wait()
        for half in range(2):
            chunk = 2 * turn + half
            gen(1 - half, jnp.minimum(chunk + 1, chunks - 1))
            w = w_ref[:, pl.ds(pl.multiple_of(chunk * kc, kc), kc)]
            norm_add(nacc_ref, w, lambda c, r, n, at: held_ref[chunk, c, r : r + n, at : at + LANES], kc)
            g = jnp.concatenate([held_ref[chunk, 0], held_ref[chunk, 1]], axis=0)
            acc_ref[...] += dot_t(y_refs[half][...], g)
        return carry

    lax.fori_loop(0, chunks // 2, pair, 0)
    part = tsub // freqs
    acc = acc_ref[...]
    swap = pltpu.roll(acc, LANES - tsub, 1)
    corr_real = acc[:cols] + swap[cols:]
    corr_imag = acc[cols:] - swap[:cols]
    lane = lax.broadcasted_iota(jnp.int32, (1, LANES), 1)
    norms = jnp.broadcast_to(norm_row(nacc_ref[...]), (8, LANES))

    def pack(dest):
        real, imag = corr_real, pltpu.roll(corr_imag, part, 1)
        for d in range(1, freqs):
            here = dest == d
            real = jnp.where(here, pltpu.roll(corr_real, LANES - d * part, 1), real)
            moved = corr_imag if d == 1 else pltpu.roll(corr_imag, LANES - (d - 1) * part, 1)
            imag = jnp.where(here, moved, imag)
        row = norms
        for d in range(1, freqs):
            row = jnp.where(dest == d, pltpu.roll(norms, LANES - d * part, 1), row)
        return jnp.concatenate(
            [jnp.where(lane < part, real, jnp.where(lane < 2 * part, imag, 0.0)), row], axis=0
        )

    keep_ref[...] = pack(freq)
    for k in range(1, freqs):
        send_ref[k - 1] = pack(lax.rem(freq + k, freqs))


def fine_final_kernel(keep_ref, *rest, freqs, n, part):
    recv_refs = rest[: freqs - 1]
    out_refs = rest[freqs - 1 :]
    x = keep_ref[...]
    for ref in recv_refs:
        x = x + ref[0]
    norm = x[n * LAGS : n * LAGS + 1]
    e = x[: n * LAGS]
    e = e * e
    e = e + pltpu.roll(e, LANES - part, 1)
    for i in range(n):
        top = jnp.max(e[i * LAGS : (i + 1) * LAGS], axis=0, keepdims=True)
        out_refs[i // CAP][i % CAP : i % CAP + 1, :] = top / norm


def params(mib=50, **kw):
    return pltpu.CompilerParams(vmem_limit_bytes=mib * 1024 * 1024, **kw)


SMEM = pl.BlockSpec(memory_space=pltpu.SMEM)
VMEM = pl.BlockSpec(memory_space=pltpu.VMEM)
HBM = pl.BlockSpec(memory_space=pltpu.HBM)


def coarse_section(info, weight, templates, blocks, banks, freqs, period):
    segs = blocks[0].shape[0]
    rows, bins = templates.shape[1], templates.shape[2]
    total = banks * segs
    cols = total * LAGS
    kc = min(1024, bins // 2)
    chunks = bins // kc
    part = rows // freqs
    kernel = functools.partial(
        coarse_kernel, blocks=len(blocks), segs=segs, banks=banks, freqs=freqs, chunks=chunks, kc=kc, period=period
    )
    return pl.pallas_call(
        kernel,
        in_specs=[
            SMEM,
            VMEM,
            HBM,
        ]
        + [VMEM for _ in blocks],
        out_shape=[
            jax.ShapeDtypeStruct((part + 8, 2 * cols), F32),
            jax.ShapeDtypeStruct((freqs - 1, part + 8, 2 * cols), F32),
        ],
        scratch_shapes=[
            *[pltpu.VMEM((banks, 2 * segs, kc), F32) for _ in range(2)],
            *[pltpu.VMEM((4, total, kc), F32) for _ in range(2)],
            *[pltpu.VMEM((2 * cols, 2 * kc), BF16) for _ in range(2)],
            pltpu.VMEM((rows, 2 * cols), F32),
            pltpu.VMEM((rows, LANES), F32),
            pltpu.VMEM((2, PAIRS, kc), F32),
            pltpu.VMEM((2, PAIRS, kc), F32),
            pltpu.VMEM((chunks, 2, rows, kc), BF16),
            pltpu.SemaphoreType.DMA((chunks,)),
        ],
        compiler_params=params(),
        cost_estimate=pl.CostEstimate(
            flops=8 * rows * bins * cols, bytes_accessed=4 * rows * bins, transcendentals=0
        ),
        name="coarse",
    )(info, weight, templates, *blocks)


def fine_section(info, weight, mult, templates, blocks, freqs, period):
    bins = templates.shape[3]
    tsub = templates.shape[2]
    n = CAP * len(blocks)
    cols = n * LAGS
    kc = min(4096, bins // 2)
    chunks = bins // kc
    kernel = functools.partial(
        fine_kernel, blocks=len(blocks), freqs=freqs, chunks=chunks, kc=kc, period=period
    )
    return pl.pallas_call(
        kernel,
        in_specs=[
            SMEM,
            VMEM,
            VMEM,
            HBM,
        ]
        + [VMEM for _ in blocks],
        out_shape=[
            jax.ShapeDtypeStruct((cols + 8, LANES), F32),
            jax.ShapeDtypeStruct((freqs - 1, cols + 8, LANES), F32),
        ],
        scratch_shapes=[
            *[pltpu.VMEM((2, n, kc), F32) for _ in range(4)],
            *[pltpu.VMEM((2 * cols, kc), BF16) for _ in range(2)],
            pltpu.VMEM((2 * cols, LANES), F32),
            pltpu.VMEM((tsub, LANES), F32),
            pltpu.VMEM((2, PAIRS, kc), F32),
            pltpu.VMEM((2, n, kc), F32),
            pltpu.VMEM((chunks, 2, tsub, kc), BF16),
            pltpu.SemaphoreType.DMA((chunks,)),
        ],
        compiler_params=params(),
        cost_estimate=pl.CostEstimate(
            flops=8 * tsub * bins * cols, bytes_accessed=4 * tsub * bins, transcendentals=0
        ),
        name="fine",
    )(info, weight, mult, templates, *blocks)


def after(value, *others):
    return lax.optimization_barrier((value, *others))[0]


def shift_permute(value, axis, count, by):
    return lax.ppermute(value, axis, [(i, (i + by) % count) for i in range(count)])


def body(
    coarse_spectra,
    fine_spectra,
    coarse_templates,
    fine_templates,
    coarse_weight,
    fine_weight,
    triggers,
    offsets,
):
    banks = lax.axis_size("bank")
    freqs = lax.axis_size("freq")
    bank = lax.axis_index("bank")
    freq = lax.axis_index("freq")
    segs = fine_spectra.shape[0]
    coarse_bins = coarse_spectra.shape[2]
    fine_bins = fine_spectra.shape[2]
    top = triggers.shape[1]
    tsub = fine_templates.shape[2]
    part = tsub // freqs
    coarse_period = 4 * coarse_bins * freqs
    fine_period = 4 * fine_bins * freqs
    zero = jnp.zeros((), jnp.int32)
    coarse_info = jnp.stack([freq * coarse_bins, bank, freq, zero]).astype(jnp.int32)
    fine_info = jnp.stack([freq * fine_bins, bank, freq, zero]).astype(jnp.int32)
    coarse_weight = coarse_weight.reshape(1, -1)
    fine_weight = fine_weight.reshape(1, -1)

    coarse_blocks = [coarse_spectra] + [
        shift_permute(coarse_spectra, "bank", banks, k) for k in range(1, banks)
    ]

    *picked, mult = pl.pallas_call(
        functools.partial(pick_kernel, banks=banks, segs=segs, top=top),
        in_specs=[SMEM, SMEM, SMEM, pl.BlockSpec(memory_space=pltpu.HBM)],
        out_shape=[jax.ShapeDtypeStruct((CAP, 2, fine_bins), BF16) for _ in range(banks)]
        + [jax.ShapeDtypeStruct((banks * CAP, LANES), jnp.int32)],
        scratch_shapes=[pltpu.SemaphoreType.DMA((banks * CAP,))],
        compiler_params=params(),
        name="pick",
    )(fine_info, triggers.T, offsets.T, fine_spectra)
    order = sorted(range(banks), key=lambda k: min(k, banks - k))
    fine_blocks = {}
    for k in order:
        fine_blocks[k] = picked[k] if k == 0 else shift_permute(picked[k], "bank", banks, k)

    def exchange(send):
        return [shift_permute(send[k - 1 : k], "freq", freqs, k) for k in range(1, freqs)]

    keep, send = coarse_section(
        coarse_info, coarse_weight, coarse_templates, coarse_blocks, banks, freqs, coarse_period
    )
    coarse_keep, coarse_received = keep, exchange(send)
    keep, send = fine_section(
        after(fine_info, coarse_keep),
        fine_weight,
        mult,
        fine_templates,
        [fine_blocks[k] for k in range(banks)],
        freqs,
        fine_period,
    )
    received = exchange(send)
    coarse_snr = pl.pallas_call(
        functools.partial(coarse_final_kernel, freqs=freqs, total=banks * segs),
        out_shape=jax.ShapeDtypeStruct((banks * segs, coarse_keep.shape[0] - 8), F32),
        compiler_params=params(16),
        name="coarse_final",
    )(after(coarse_keep, keep), *coarse_received)
    results = pl.pallas_call(
        functools.partial(fine_final_kernel, freqs=freqs, n=CAP * banks, part=part),
        out_shape=[jax.ShapeDtypeStruct((CAP, LANES), F32) for _ in range(banks)],
        compiler_params=params(8),
        name="fine_final",
    )(after(keep, coarse_snr), *received)
    back = [
        results[k] if k == 0 else shift_permute(results[k], "bank", banks, banks - k)
        for k in range(banks)
    ]
    fine_snr = pl.pallas_call(
        functools.partial(place_kernel, banks=banks, segs=segs, top=top),
        in_specs=[SMEM, SMEM] + [pl.BlockSpec(memory_space=pltpu.VMEM) for _ in range(banks)],
        out_shape=jax.ShapeDtypeStruct((segs, top, part), F32),
        scratch_shapes=[pltpu.VMEM((banks * CAP, LANES), F32)],
        compiler_params=params(8),
        name="place",
    )(fine_info, triggers.T, *back)
    return (coarse_snr.T, fine_snr)


def solution(mesh):
    return sharded(mesh)


def sharded(mesh):
    return jax.shard_map(
        body,
        mesh=mesh,
        in_specs=(
            P(("groups", "seg", "bank"), None, "freq"),
            P(("groups", "seg", "bank"), None, "freq"),
            P(None, "bank", "freq"),
            P(None, "bank", None, "freq"),
            P(("groups", "freq")),
            P(("groups", "freq")),
            P(("groups", "seg"), None),
            P(("groups", "seg"), None),
        ),
        out_specs=(
            P(("bank", "freq"), ("groups", "seg")),
            P(("groups", "seg", "bank"), None, "freq"),
        ),
        check_vma=False,
    )
```

```python
import functools
import math

import jax
import jax.numpy as jnp
from jax import lax
from jax.experimental import pallas as pl
from jax.experimental.pallas import tpu as pltpu
from jax.sharding import PartitionSpec as P


CAP = 2
LAGS = 16
PAIRS = LAGS // 2
CSTRIDE = 2047
LANES = 128
F32 = jnp.float32
BF16 = jnp.bfloat16


def sincos(counts, period):
    half = period // 2
    signed = ((counts + half) & (period - 1)) - half
    x = signed.astype(F32) * (1.0 / period)
    u = x * x
    p = math.pi
    s = -(p**11) / 39916800.0
    for a in (p**9 / 362880.0, -(p**7) / 5040.0, p**5 / 120.0, -(p**3) / 6.0, p):
        s = s * u + a
    s = s * x
    c = p**12 / 479001600.0
    for a in (-(p**10) / 3628800.0, p**8 / 40320.0, -(p**6) / 720.0, p**4 / 24.0, -(p**2) / 2.0, 1.0):
        c = c * u + a
    return 1.0 - 2.0 * s * s, 2.0 * s * c


def dot_t(a, b):
    return lax.dot_general(a, b, (((1,), (1,)), ((), ())), preferred_element_type=F32)


def rotate(c, s, dc, ds):
    return c * dc - s * ds, s * dc + c * ds


def norm_add(acc_ref, w_ref, held_ref, chunk, turn, turns):
    rows = acc_ref.shape[0]
    bins = held_ref.shape[3]
    count = max(rows // turns, 16)
    r = turn * count
    if r >= rows:
        return
    n = acc_ref[r : r + count, :]
    for lo in range(0, bins, LANES):
        re = held_ref[chunk, 0, r : r + count, lo : lo + LANES].astype(F32)
        im = held_ref[chunk, 1, r : r + count, lo : lo + LANES].astype(F32)
        w = w_ref[:, pl.ds(pl.multiple_of(chunk * bins + lo, LANES), LANES)]
        n = n + (re * re + im * im) * w
    acc_ref[r : r + count, :] = n


def norm_row(n):
    if n.shape[0] < LANES:
        n = jnp.concatenate([n, jnp.zeros((LANES - n.shape[0], LANES), F32)], axis=0)
    return jnp.sum(n.T, axis=0, keepdims=True)


def coarse_kernel(
    info_ref, w_ref, h_ref, *rest, blocks, segs, banks, freqs, chunks, kc, period
):
    spec_refs = rest[:blocks]
    keep_ref, send_ref = rest[blocks : blocks + 2]
    a_refs, b_refs, y_refs = (rest[blocks + i : blocks + i + 2] for i in (2, 4, 6))
    acc_ref, nacc_ref, tab_ref, ctr_ref, held_ref, sems = rest[blocks + 8 :]
    base = info_ref[0]
    bank = info_ref[1]
    freq = info_ref[2]
    total = banks * segs
    cols = total * LAGS

    def fetch(chunk):
        at = pl.ds(pl.multiple_of(chunk * kc, kc), kc)
        return pltpu.make_async_copy(h_ref.at[:, :, at], held_ref.at[chunk], sems.at[chunk])

    for chunk in range(chunks):
        fetch(chunk).start()

    def gen(which, chunk, beside=lambda i: None):
        a_ref, b_ref, y_ref = a_refs[which], b_refs[which], y_refs[which]
        shift = pl.multiple_of(chunk * kc, kc)
        w = w_ref[:, pl.ds(shift, kc)]
        for k in range(blocks):
            source = lax.rem(bank - k + banks, banks)
            for i in range(segs):
                a_ref[source, 2 * i : 2 * i + 2, :] = spec_refs[k][i, :, pl.ds(shift, kc)].astype(F32) * w
        odd = 2 * lax.broadcasted_iota(jnp.int32, (PAIRS, LANES), 0) + 1
        dc, ds = sincos(shift * odd * CSTRIDE, period)
        ec, es = sincos(jnp.full((PAIRS, LANES), shift * (15 * CSTRIDE), jnp.int32), period)
        for lo in range(0, kc, LANES):
            lanes = slice(lo, lo + LANES)
            c, s = rotate(ctr_ref[0, :, lanes], ctr_ref[1, :, lanes], ec, es)
            for b in range(0, total, 4):
                re, im = (
                    jnp.concatenate(
                        [a_ref[(b + i) // segs, 2 * ((b + i) % segs) + c : 2 * ((b + i) % segs) + c + 1, lanes] for i in range(4)],
                        axis=0,
                    )
                    for c in range(2)
                )
                b_ref[0, b : b + 4, lanes] = re * c[:4] - im * s[:4]
                b_ref[1, b : b + 4, lanes] = re * s[:4] + im * c[:4]
            c, s = rotate(tab_ref[0, :, lanes], tab_ref[1, :, lanes], dc, ds)
            b_ref[2, :PAIRS, lanes] = c
            b_ref[3, :PAIRS, lanes] = s
            re = b_ref[0, :, lanes]
            im = b_ref[1, :, lanes]
            for m in range(PAIRS):
                cm = b_ref[2, m : m + 1, lanes]
                sm = b_ref[3, m : m + 1, lanes]
                rc = re * cm
                js = im * sm
                jc = im * cm
                rs = re * sm
                for sign, (yr, yi) in enumerate(((rc - js, jc + rs), (rc + js, jc - rs))):
                    at = (2 * m + sign) * total
                    yr = yr.astype(BF16)
                    yi = yi.astype(BF16)
                    y_ref[at : at + total, lo : lo + LANES] = yr
                    y_ref[at : at + total, kc + lo : kc + lo + LANES] = yi
                    y_ref[cols + at : cols + at + total, lo : lo + LANES] = yi
                    y_ref[cols + at : cols + at + total, kc + lo : kc + lo + LANES] = -yr
            beside(lo // LANES)

    ids = base + lax.broadcasted_iota(jnp.int32, (PAIRS, kc), 1)
    odd = 2 * lax.broadcasted_iota(jnp.int32, (PAIRS, kc), 0) + 1
    c, s = sincos(ids * odd * CSTRIDE, period)
    tab_ref[0] = c
    tab_ref[1] = s
    c, s = sincos(ids * (15 * CSTRIDE), period)
    ctr_ref[0] = c
    ctr_ref[1] = s
    acc_ref[...] = jnp.zeros_like(acc_ref)
    nacc_ref[...] = jnp.zeros_like(nacc_ref)
    gen(0, jnp.int32(0))

    def pair(turn, carry):
        fetch(2 * turn).wait()
        fetch(2 * turn + 1).wait()
        for half in range(2):
            chunk = 2 * turn + half
            beside = functools.partial(norm_add, nacc_ref, w_ref, held_ref, chunk, turns=kc // LANES)
            gen(1 - half, jnp.minimum(chunk + 1, chunks - 1), beside)
            h = jnp.concatenate([held_ref[chunk, 0], held_ref[chunk, 1]], axis=1)
            acc_ref[...] += dot_t(h, y_refs[half][...])
        return carry

    lax.fori_loop(0, chunks // 2, pair, 0)
    part = acc_ref.shape[0] // freqs
    size = min(part, LANES)

    def lay(ref, dest):
        first = pl.multiple_of(dest * part, part)
        ref[:part, :] = acc_ref[pl.ds(first, part), :]
        for r in range(0, part, size):
            row = norm_row(nacc_ref[pl.ds(first + r, size), :])
            ref[part : part + 8, r : r + LANES] = jnp.broadcast_to(row, (8, LANES))

    lay(keep_ref, freq)
    for k in range(1, freqs):
        lay(send_ref.at[k - 1], lax.rem(freq + k, freqs))


def coarse_final_kernel(keep_ref, *rest, freqs, total):
    recv_refs = rest[: freqs - 1]
    out_ref = rest[freqs - 1]
    part = keep_ref.shape[0] - 8
    cols = total * LAGS
    corr = keep_ref[...]
    for ref in recv_refs:
        corr = corr + ref[0]
    norms = corr[part : part + 1]
    cr = corr[:part, :cols]
    ci = corr[:part, cols:]
    e = cr * cr + ci * ci
    width = cols
    while width > max(total, LANES):
        width //= 2
        e = jnp.maximum(e[:, :width], e[:, width:])
    while width > total:
        width //= 2
        e = jnp.maximum(e, pltpu.roll(e, LANES - width, 1))
    size = min(part, LANES)
    for r in range(0, part, size):
        rows = e[r : r + size]
        if size < LANES:
            rows = jnp.concatenate([rows, jnp.zeros((LANES - size, LANES), F32)], axis=0)
        out = rows.T[:total] / norms[:, r : r + LANES]
        out_ref[:, r : r + size] = out[:, :size]


def ranked_pairs(trig_ref, first, segs, top, target):
    taken = jnp.int32(0)
    found = [jnp.int32(0) for _ in range(CAP)]
    for p in range(segs * top):
        hit = (trig_ref[p % top, first + p // top] == target).astype(jnp.int32)
        for c in range(CAP):
            found[c] = jnp.where(jnp.logical_and(hit == 1, taken == c), p, found[c])
        taken = taken + hit
    return taken, found


def pick_kernel(info_ref, trig_ref, off_ref, spec_ref, *rest, banks, segs, top):
    out_refs = rest[:banks]
    mult_ref, sems = rest[banks:]
    bank = info_ref[1]
    copies = []
    for k in range(banks):
        k = (k + 1) % banks
        dest = lax.rem(bank + k, banks)
        _, found = ranked_pairs(trig_ref, bank * segs, segs, top, dest)
        for c in range(CAP):
            copy = pltpu.make_async_copy(
                spec_ref.at[found[c] // top], out_refs[k].at[c], sems.at[k * CAP + c]
            )
            copy.start()
            copies.append(copy)
    line = lax.broadcasted_iota(jnp.int32, mult_ref.shape, 0)
    mult = jnp.zeros(mult_ref.shape, jnp.int32)
    for k in range(banks):
        source = lax.rem(bank - k + banks, banks)
        _, found = ranked_pairs(trig_ref, source * segs, segs, top, bank)
        for c in range(CAP):
            offset = off_ref[lax.rem(found[c], top), source * segs + found[c] // top]
            mult = jnp.where(line == k * CAP + c, 2 * offset + (LAGS - 1), mult)
    mult_ref[...] = mult
    for copy in copies:
        copy.wait()


def place_kernel(info_ref, trig_ref, *rest, banks, segs, top):
    back_refs = rest[:banks]
    out_ref, all_ref = rest[banks:]
    bank = info_ref[1]
    part = out_ref.shape[2]
    for k in range(banks):
        all_ref[CAP * k : CAP * (k + 1), :] = back_refs[k][...]
    for p in range(segs * top):
        target = trig_ref[p % top, bank * segs + p // top]
        rank = jnp.int32(0)
        for q in range(p):
            rank = rank + (trig_ref[q % top, bank * segs + q // top] == target).astype(jnp.int32)
        at = lax.rem(target - bank + banks, banks) * CAP + jnp.minimum(rank, CAP - 1)
        out_ref[p // top, p % top : p % top + 1, :] = all_ref[pl.ds(at, 1), :][:, :part]


def fine_kernel(info_ref, w_ref, mult_ref, g_ref, *rest, blocks, freqs, chunks, kc, period):
    slot_refs = rest[:blocks]
    keep_ref, send_ref = rest[blocks : blocks + 2]
    a_refs, b_refs, y_refs = (rest[blocks + i : blocks + i + 2] for i in (2, 4, 6))
    acc_ref, nacc_ref, tab_ref, ctr_ref, held_ref, sems = rest[blocks + 8 :]
    base = info_ref[0]
    freq = info_ref[2]
    n = blocks * CAP
    cols = n * LAGS
    tsub = g_ref.shape[2]

    def fetch(chunk):
        at = pl.ds(pl.multiple_of(chunk * kc, kc), kc)
        return pltpu.make_async_copy(g_ref.at[:, 0, :, at], held_ref.at[chunk], sems.at[chunk])

    for chunk in range(chunks):
        fetch(chunk).start()

    def gen(which, chunk, beside=lambda i: None):
        a_ref, b_ref, y_ref = a_refs[which], b_refs[which], y_refs[which]
        shift = pl.multiple_of(chunk * kc, kc)
        w = w_ref[:, pl.ds(shift, kc)]
        for k in range(blocks):
            for i in range(CAP):
                x = slot_refs[k][i, :, pl.ds(shift, kc)].astype(F32) * w
                a_ref[0, CAP * k + i : CAP * k + i + 1, :] = x[0:1]
                a_ref[1, CAP * k + i : CAP * k + i + 1, :] = x[1:2]
        odd = 2 * lax.broadcasted_iota(jnp.int32, (PAIRS, LANES), 0) + 1
        dc, ds = sincos(shift * odd, period)
        ec, es = sincos(shift * mult_ref[...], period)
        for lo in range(0, kc, LANES):
            lanes = slice(lo, lo + LANES)
            c, s = rotate(ctr_ref[0, :, lanes], ctr_ref[1, :, lanes], ec, es)
            re = a_ref[0, :, lanes]
            im = a_ref[1, :, lanes]
            b_ref[0, :, lanes] = re * c - im * s
            b_ref[1, :, lanes] = re * s + im * c
            c, s = rotate(tab_ref[0, :, lanes], tab_ref[1, :, lanes], dc, ds)
            for i in range(n):
                re = b_ref[0, i : i + 1, lanes]
                im = b_ref[1, i : i + 1, lanes]
                rc = re * c
                js = im * s
                jc = im * c
                rs = re * s
                at = i * LAGS
                y_ref[at : at + LAGS, lanes] = jnp.concatenate([rc - js, rc + js], axis=0).astype(BF16)
                y_ref[cols + at : cols + at + LAGS, lanes] = jnp.concatenate(
                    [jc + rs, jc - rs], axis=0
                ).astype(BF16)
            beside(lo // LANES)

    ids = base + lax.broadcasted_iota(jnp.int32, (PAIRS, kc), 1)
    odd = 2 * lax.broadcasted_iota(jnp.int32, (PAIRS, kc), 0) + 1
    c, s = sincos(ids * odd, period)
    tab_ref[0] = c
    tab_ref[1] = s
    ids = base + lax.broadcasted_iota(jnp.int32, (n, kc), 1)
    c, s = sincos(ids * mult_ref[:, 0:1], period)
    ctr_ref[0] = c
    ctr_ref[1] = s
    acc_ref[...] = jnp.zeros_like(acc_ref)
    nacc_ref[...] = jnp.zeros_like(nacc_ref)
    gen(0, jnp.int32(0))

    def pair(turn, carry):
        fetch(2 * turn).wait()
        fetch(2 * turn + 1).wait()
        for half in range(2):
            chunk = 2 * turn + half
            beside = functools.partial(norm_add, nacc_ref, w_ref, held_ref, chunk, turns=kc // LANES)
            gen(1 - half, jnp.minimum(chunk + 1, chunks - 1), beside)
            g = jnp.concatenate([held_ref[chunk, 0], held_ref[chunk, 1]], axis=0)
            acc_ref[...] += dot_t(y_refs[half][...], g)
        return carry

    lax.fori_loop(0, chunks // 2, pair, 0)
    part = tsub // freqs
    acc = acc_ref[...]
    swap = pltpu.roll(acc, LANES - tsub, 1)
    corr_real = acc[:cols] + swap[cols:]
    corr_imag = acc[cols:] - swap[:cols]
    lane = lax.broadcasted_iota(jnp.int32, (1, LANES), 1)
    norms = jnp.broadcast_to(norm_row(nacc_ref[...]), (8, LANES))

    def pack(dest):
        real, imag = corr_real, pltpu.roll(corr_imag, part, 1)
        for d in range(1, freqs):
            here = dest == d
            real = jnp.where(here, pltpu.roll(corr_real, LANES - d * part, 1), real)
            moved = corr_imag if d == 1 else pltpu.roll(corr_imag, LANES - (d - 1) * part, 1)
            imag = jnp.where(here, moved, imag)
        row = norms
        for d in range(1, freqs):
            row = jnp.where(dest == d, pltpu.roll(norms, LANES - d * part, 1), row)
        return jnp.concatenate(
            [jnp.where(lane < part, real, jnp.where(lane < 2 * part, imag, 0.0)), row], axis=0
        )

    keep_ref[...] = pack(freq)
    for k in range(1, freqs):
        send_ref[k - 1] = pack(lax.rem(freq + k, freqs))


def fine_final_kernel(keep_ref, *rest, freqs, n, part):
    recv_refs = rest[: freqs - 1]
    out_refs = rest[freqs - 1 :]
    x = keep_ref[...]
    for ref in recv_refs:
        x = x + ref[0]
    norm = x[n * LAGS : n * LAGS + 1]
    e = x[: n * LAGS]
    e = e * e
    e = e + pltpu.roll(e, LANES - part, 1)
    for i in range(n):
        top = jnp.max(e[i * LAGS : (i + 1) * LAGS], axis=0, keepdims=True)
        out_refs[i // CAP][i % CAP : i % CAP + 1, :] = top / norm


def params(mib=50, **kw):
    return pltpu.CompilerParams(vmem_limit_bytes=mib * 1024 * 1024, **kw)


SMEM = pl.BlockSpec(memory_space=pltpu.SMEM)
VMEM = pl.BlockSpec(memory_space=pltpu.VMEM)
HBM = pl.BlockSpec(memory_space=pltpu.HBM)


def coarse_section(info, weight, templates, blocks, banks, freqs, period):
    segs = blocks[0].shape[0]
    rows, bins = templates.shape[1], templates.shape[2]
    total = banks * segs
    cols = total * LAGS
    kc = min(1024, bins // 2)
    chunks = bins // kc
    part = rows // freqs
    kernel = functools.partial(
        coarse_kernel, blocks=len(blocks), segs=segs, banks=banks, freqs=freqs, chunks=chunks, kc=kc, period=period
    )
    return pl.pallas_call(
        kernel,
        in_specs=[
            SMEM,
            VMEM,
            HBM,
        ]
        + [VMEM for _ in blocks],
        out_shape=[
            jax.ShapeDtypeStruct((part + 8, 2 * cols), F32),
            jax.ShapeDtypeStruct((freqs - 1, part + 8, 2 * cols), F32),
        ],
        scratch_shapes=[
            *[pltpu.VMEM((banks, 2 * segs, kc), F32) for _ in range(2)],
            *[pltpu.VMEM((4, total, kc), F32) for _ in range(2)],
            *[pltpu.VMEM((2 * cols, 2 * kc), BF16) for _ in range(2)],
            pltpu.VMEM((rows, 2 * cols), F32),
            pltpu.VMEM((rows, LANES), F32),
            pltpu.VMEM((2, PAIRS, kc), F32),
            pltpu.VMEM((2, PAIRS, kc), F32),
            pltpu.VMEM((chunks, 2, rows, kc), BF16),
            pltpu.SemaphoreType.DMA((chunks,)),
        ],
        compiler_params=params(),
        cost_estimate=pl.CostEstimate(
            flops=8 * rows * bins * cols, bytes_accessed=4 * rows * bins, transcendentals=0
        ),
        name="coarse",
    )(info, weight, templates, *blocks)


def fine_section(info, weight, mult, templates, blocks, freqs, period):
    bins = templates.shape[3]
    tsub = templates.shape[2]
    n = CAP * len(blocks)
    cols = n * LAGS
    kc = min(4096, bins // 2)
    chunks = bins // kc
    kernel = functools.partial(
        fine_kernel, blocks=len(blocks), freqs=freqs, chunks=chunks, kc=kc, period=period
    )
    return pl.pallas_call(
        kernel,
        in_specs=[
            SMEM,
            VMEM,
            VMEM,
            HBM,
        ]
        + [VMEM for _ in blocks],
        out_shape=[
            jax.ShapeDtypeStruct((cols + 8, LANES), F32),
            jax.ShapeDtypeStruct((freqs - 1, cols + 8, LANES), F32),
        ],
        scratch_shapes=[
            *[pltpu.VMEM((2, n, kc), F32) for _ in range(4)],
            *[pltpu.VMEM((2 * cols, kc), BF16) for _ in range(2)],
            pltpu.VMEM((2 * cols, LANES), F32),
            pltpu.VMEM((tsub, LANES), F32),
            pltpu.VMEM((2, PAIRS, kc), F32),
            pltpu.VMEM((2, n, kc), F32),
            pltpu.VMEM((chunks, 2, tsub, kc), BF16),
            pltpu.SemaphoreType.DMA((chunks,)),
        ],
        compiler_params=params(),
        cost_estimate=pl.CostEstimate(
            flops=8 * tsub * bins * cols, bytes_accessed=4 * tsub * bins, transcendentals=0
        ),
        name="fine",
    )(info, weight, mult, templates, *blocks)


def after(value, *others):
    return lax.optimization_barrier((value, *others))[0]


def shift_permute(value, axis, count, by):
    return lax.ppermute(value, axis, [(i, (i + by) % count) for i in range(count)])


def body(
    coarse_spectra,
    fine_spectra,
    coarse_templates,
    fine_templates,
    coarse_weight,
    fine_weight,
    triggers,
    offsets,
):
    banks = lax.axis_size("bank")
    freqs = lax.axis_size("freq")
    bank = lax.axis_index("bank")
    freq = lax.axis_index("freq")
    segs = fine_spectra.shape[0]
    coarse_bins = coarse_spectra.shape[2]
    fine_bins = fine_spectra.shape[2]
    top = triggers.shape[1]
    tsub = fine_templates.shape[2]
    part = tsub // freqs
    coarse_period = 4 * coarse_bins * freqs
    fine_period = 4 * fine_bins * freqs
    zero = jnp.zeros((), jnp.int32)
    coarse_info = jnp.stack([freq * coarse_bins, bank, freq, zero]).astype(jnp.int32)
    fine_info = jnp.stack([freq * fine_bins, bank, freq, zero]).astype(jnp.int32)
    coarse_weight = coarse_weight.reshape(1, -1)
    fine_weight = fine_weight.reshape(1, -1)

    coarse_blocks = [coarse_spectra] + [
        shift_permute(coarse_spectra, "bank", banks, k) for k in range(1, banks)
    ]

    *picked, mult = pl.pallas_call(
        functools.partial(pick_kernel, banks=banks, segs=segs, top=top),
        in_specs=[SMEM, SMEM, SMEM, pl.BlockSpec(memory_space=pltpu.HBM)],
        out_shape=[jax.ShapeDtypeStruct((CAP, 2, fine_bins), BF16) for _ in range(banks)]
        + [jax.ShapeDtypeStruct((banks * CAP, LANES), jnp.int32)],
        scratch_shapes=[pltpu.SemaphoreType.DMA((banks * CAP,))],
        compiler_params=params(),
        name="pick",
    )(fine_info, triggers.T, offsets.T, fine_spectra)
    order = sorted(range(banks), key=lambda k: min(k, banks - k))
    fine_blocks = {}
    for place, k in enumerate(order):
        block = picked[k] if place < 2 else after(picked[k], *coarse_blocks)
        fine_blocks[k] = block if k == 0 else shift_permute(block, "bank", banks, k)

    def exchange(send):
        return [shift_permute(send[k - 1 : k], "freq", freqs, k) for k in range(1, freqs)]

    keep, send = coarse_section(
        coarse_info, coarse_weight, coarse_templates, coarse_blocks, banks, freqs, coarse_period
    )
    coarse_keep, coarse_received = keep, exchange(send)
    keep, send = fine_section(
        after(fine_info, coarse_keep),
        fine_weight,
        mult,
        fine_templates,
        [fine_blocks[k] for k in range(banks)],
        freqs,
        fine_period,
    )
    received = exchange(send)
    coarse_snr = pl.pallas_call(
        functools.partial(coarse_final_kernel, freqs=freqs, total=banks * segs),
        out_shape=jax.ShapeDtypeStruct((banks * segs, coarse_keep.shape[0] - 8), F32),
        compiler_params=params(16),
        name="coarse_final",
    )(after(coarse_keep, keep), *coarse_received)
    results = pl.pallas_call(
        functools.partial(fine_final_kernel, freqs=freqs, n=CAP * banks, part=part),
        out_shape=[jax.ShapeDtypeStruct((CAP, LANES), F32) for _ in range(banks)],
        compiler_params=params(8),
        name="fine_final",
    )(after(keep, coarse_snr), *received)
    back = [
        results[k] if k == 0 else shift_permute(results[k], "bank", banks, banks - k)
        for k in range(banks)
    ]
    fine_snr = pl.pallas_call(
        functools.partial(place_kernel, banks=banks, segs=segs, top=top),
        in_specs=[SMEM, SMEM] + [pl.BlockSpec(memory_space=pltpu.VMEM) for _ in range(banks)],
        out_shape=jax.ShapeDtypeStruct((segs, top, part), F32),
        scratch_shapes=[pltpu.VMEM((banks * CAP, LANES), F32)],
        compiler_params=params(8),
        name="place",
    )(fine_info, triggers.T, *back)
    return (coarse_snr.T, fine_snr)


def solution(mesh):
    return sharded(mesh)


def sharded(mesh):
    return jax.shard_map(
        body,
        mesh=mesh,
        in_specs=(
            P(("groups", "seg", "bank"), None, "freq"),
            P(("groups", "seg", "bank"), None, "freq"),
            P(None, "bank", "freq"),
            P(None, "bank", None, "freq"),
            P(("groups", "freq")),
            P(("groups", "freq")),
            P(("groups", "seg"), None),
            P(("groups", "seg"), None),
        ),
        out_specs=(
            P(("bank", "freq"), ("groups", "seg")),
            P(("groups", "seg", "bank"), None, "freq"),
        ),
        check_vma=False,
    )
```

```python
import functools
import math

import jax
import jax.numpy as jnp
from jax import lax
from jax.experimental import pallas as pl
from jax.experimental.pallas import tpu as pltpu
from jax.sharding import PartitionSpec as P


CAP = 2
LAGS = 16
PAIRS = LAGS // 2
CSTRIDE = 2047
LANES = 128
F32 = jnp.float32
BF16 = jnp.bfloat16


def sincos(counts, period):
    half = period // 2
    signed = ((counts + half) & (period - 1)) - half
    x = signed.astype(F32) * (1.0 / period)
    u = x * x
    p = math.pi
    s = -(p**11) / 39916800.0
    for a in (p**9 / 362880.0, -(p**7) / 5040.0, p**5 / 120.0, -(p**3) / 6.0, p):
        s = s * u + a
    s = s * x
    c = p**12 / 479001600.0
    for a in (-(p**10) / 3628800.0, p**8 / 40320.0, -(p**6) / 720.0, p**4 / 24.0, -(p**2) / 2.0, 1.0):
        c = c * u + a
    return 1.0 - 2.0 * s * s, 2.0 * s * c


def dot_t(a, b):
    return lax.dot_general(a, b, (((1,), (1,)), ((), ())), preferred_element_type=F32)


def rotate(c, s, dc, ds):
    return c * dc - s * ds, s * dc + c * ds


def norm_add(acc_ref, w_ref, held_ref, chunk, turn, turns):
    rows = acc_ref.shape[0]
    bins = held_ref.shape[3]
    count = max(rows // turns, 16)
    r = turn * count
    if r >= rows:
        return
    n = acc_ref[r : r + count, :]
    for lo in range(0, bins, LANES):
        re = held_ref[chunk, 0, r : r + count, lo : lo + LANES].astype(F32)
        im = held_ref[chunk, 1, r : r + count, lo : lo + LANES].astype(F32)
        w = w_ref[:, pl.ds(pl.multiple_of(chunk * bins + lo, LANES), LANES)]
        n = n + (re * re + im * im) * w
    acc_ref[r : r + count, :] = n


def norm_row(n):
    if n.shape[0] < LANES:
        n = jnp.concatenate([n, jnp.zeros((LANES - n.shape[0], LANES), F32)], axis=0)
    return jnp.sum(n.T, axis=0, keepdims=True)


def coarse_kernel(
    info_ref, w_ref, h_ref, *rest, blocks, segs, banks, freqs, chunks, kc, period
):
    spec_refs = rest[:blocks]
    keep_ref, send_ref = rest[blocks : blocks + 2]
    a_refs, b_refs, y_refs = (rest[blocks + i : blocks + i + 2] for i in (2, 4, 6))
    acc_ref, tab_ref, ctr_ref, held_ref, sems = rest[blocks + 8 :]
    base = info_ref[0]
    bank = info_ref[1]
    freq = info_ref[2]
    total = banks * segs
    cols = total * LAGS

    def fetch(chunk):
        at = pl.ds(pl.multiple_of(chunk * kc, kc), kc)
        return pltpu.make_async_copy(h_ref.at[:, :, at], held_ref.at[chunk], sems.at[chunk])

    for chunk in range(chunks):
        fetch(chunk).start()

    def gen(which, chunk):
        a_ref, b_ref, y_ref = a_refs[which], b_refs[which], y_refs[which]
        shift = pl.multiple_of(chunk * kc, kc)
        w = w_ref[:, pl.ds(shift, kc)]
        for k in range(blocks):
            source = lax.rem(bank - k + banks, banks)
            for i in range(segs):
                a_ref[source, 2 * i : 2 * i + 2, :] = spec_refs[k][i, :, pl.ds(shift, kc)].astype(F32) * w
        odd = 2 * lax.broadcasted_iota(jnp.int32, (PAIRS, LANES), 0) + 1
        dc, ds = sincos(shift * odd * CSTRIDE, period)
        ec, es = sincos(jnp.full((PAIRS, LANES), shift * (15 * CSTRIDE), jnp.int32), period)
        for lo in range(0, kc, LANES):
            lanes = slice(lo, lo + LANES)
            c, s = rotate(ctr_ref[0, :, lanes], ctr_ref[1, :, lanes], ec, es)
            for b in range(0, total, 4):
                re, im = (
                    jnp.concatenate(
                        [a_ref[(b + i) // segs, 2 * ((b + i) % segs) + c : 2 * ((b + i) % segs) + c + 1, lanes] for i in range(4)],
                        axis=0,
                    )
                    for c in range(2)
                )
                b_ref[0, b : b + 4, lanes] = re * c[:4] - im * s[:4]
                b_ref[1, b : b + 4, lanes] = re * s[:4] + im * c[:4]
            c, s = rotate(tab_ref[0, :, lanes], tab_ref[1, :, lanes], dc, ds)
            b_ref[2, :PAIRS, lanes] = c
            b_ref[3, :PAIRS, lanes] = s
            re = b_ref[0, :, lanes]
            im = b_ref[1, :, lanes]
            for m in range(PAIRS):
                cm = b_ref[2, m : m + 1, lanes]
                sm = b_ref[3, m : m + 1, lanes]
                rc = re * cm
                js = im * sm
                jc = im * cm
                rs = re * sm
                for sign, (yr, yi) in enumerate(((rc - js, jc + rs), (rc + js, jc - rs))):
                    at = (2 * m + sign) * total
                    yr = yr.astype(BF16)
                    yi = yi.astype(BF16)
                    y_ref[at : at + total, lo : lo + LANES] = yr
                    y_ref[at : at + total, kc + lo : kc + lo + LANES] = yi
                    y_ref[cols + at : cols + at + total, lo : lo + LANES] = yi
                    y_ref[cols + at : cols + at + total, kc + lo : kc + lo + LANES] = -yr

    ids = base + lax.broadcasted_iota(jnp.int32, (PAIRS, kc), 1)
    odd = 2 * lax.broadcasted_iota(jnp.int32, (PAIRS, kc), 0) + 1
    c, s = sincos(ids * odd * CSTRIDE, period)
    tab_ref[0] = c
    tab_ref[1] = s
    c, s = sincos(ids * (15 * CSTRIDE), period)
    ctr_ref[0] = c
    ctr_ref[1] = s
    acc_ref[...] = jnp.zeros_like(acc_ref)
    gen(0, jnp.int32(0))

    def pair(turn, carry):
        fetch(2 * turn).wait()
        fetch(2 * turn + 1).wait()
        for half in range(2):
            chunk = 2 * turn + half
            gen(1 - half, jnp.minimum(chunk + 1, chunks - 1))
            h = jnp.concatenate([held_ref[chunk, 0], held_ref[chunk, 1]], axis=1)
            acc_ref[...] += dot_t(h, y_refs[half][...])
        return carry

    lax.fori_loop(0, chunks // 2, pair, 0)
    part = acc_ref.shape[0] // freqs
    keep_ref[...] = acc_ref[pl.ds(pl.multiple_of(freq * part, part), part), :]
    for k in range(1, freqs):
        dest = pl.multiple_of(lax.rem(freq + k, freqs) * part, part)
        send_ref[k - 1] = acc_ref[pl.ds(dest, part), :]


def norm_kernel(
    info_ref, cw_ref, fw_ref, h_ref, g_ref, keep_ref, send_ref, c_ref, f_ref, h_held, g_held, h_sems, g_sems, *, freqs
):
    chunks, _, rows, kc = h_held.shape
    tsub, kf = g_held.shape[2:]

    def fetch(i):
        at = pl.ds(pl.multiple_of(i * kc, kc), kc)
        yield pltpu.make_async_copy(h_ref.at[:, :, at], h_held.at[i], h_sems.at[i])
        at = pl.ds(pl.multiple_of(i * kf, kf), kf)
        yield pltpu.make_async_copy(g_ref.at[:, 0, :, at], g_held.at[i], g_sems.at[i])

    for i in range(chunks):
        for copy in fetch(i):
            copy.start()
    c_ref[...] = jnp.zeros_like(c_ref)
    f_ref[...] = jnp.zeros_like(f_ref)

    def turn(i, carry):
        for copy in fetch(i):
            copy.wait()
        for t in range(8):
            norm_add(c_ref, cw_ref, h_held, i, t, 8)
        for t in range(4):
            norm_add(f_ref, fw_ref, g_held, i, t, 4)
        return carry

    lax.fori_loop(0, chunks, turn, 0)
    part = rows // freqs
    fine_part = tsub // freqs
    size = min(part, LANES)

    def lay(ref, dest):
        ref[...] = jnp.zeros_like(ref)
        for r in range(0, part, size):
            row = norm_row(c_ref[pl.ds(pl.multiple_of(dest * part + r, size), size), :])
            ref[r // size : r // size + 1, :] = row
        row = norm_row(f_ref[pl.ds(pl.multiple_of(dest * fine_part, fine_part), fine_part), :])
        ref[part // size : part // size + 1, :] = row

    lay(keep_ref, info_ref[2])
    for k in range(1, freqs):
        lay(send_ref.at[k - 1], lax.rem(info_ref[2] + k, freqs))


def coarse_final_kernel(keep_ref, norm_ref, *rest, freqs, total):
    recv_refs = rest[: 2 * (freqs - 1)]
    out_ref = rest[2 * (freqs - 1)]
    part = keep_ref.shape[0]
    cols = total * LAGS
    corr = keep_ref[...]
    norms = norm_ref[...]
    for k in range(freqs - 1):
        corr = corr + recv_refs[2 * k][0]
        norms = norms + recv_refs[2 * k + 1][0]
    cr = corr[:part, :cols]
    ci = corr[:part, cols:]
    e = cr * cr + ci * ci
    width = cols
    while width > max(total, LANES):
        width //= 2
        e = jnp.maximum(e[:, :width], e[:, width:])
    while width > total:
        width //= 2
        e = jnp.maximum(e, pltpu.roll(e, LANES - width, 1))
    size = min(part, LANES)
    for r in range(0, part, size):
        rows = e[r : r + size]
        if size < LANES:
            rows = jnp.concatenate([rows, jnp.zeros((LANES - size, LANES), F32)], axis=0)
        out = rows.T[:total] / norms[r // size : r // size + 1]
        out_ref[:, r : r + size] = out[:, :size]


def ranked_pairs(trig_ref, first, segs, top, target):
    taken = jnp.int32(0)
    found = [jnp.int32(0) for _ in range(CAP)]
    for p in range(segs * top):
        hit = (trig_ref[p % top, first + p // top] == target).astype(jnp.int32)
        for c in range(CAP):
            found[c] = jnp.where(jnp.logical_and(hit == 1, taken == c), p, found[c])
        taken = taken + hit
    return taken, found


def pick_kernel(info_ref, trig_ref, off_ref, spec_ref, *rest, banks, segs, top):
    out_refs = rest[:banks]
    mult_ref, sems = rest[banks:]
    bank = info_ref[1]
    copies = []
    for k in range(banks):
        k = (k + 1) % banks
        dest = lax.rem(bank + k, banks)
        _, found = ranked_pairs(trig_ref, bank * segs, segs, top, dest)
        for c in range(CAP):
            copy = pltpu.make_async_copy(
                spec_ref.at[found[c] // top], out_refs[k].at[c], sems.at[k * CAP + c]
            )
            copy.start()
            copies.append(copy)
    line = lax.broadcasted_iota(jnp.int32, mult_ref.shape, 0)
    mult = jnp.zeros(mult_ref.shape, jnp.int32)
    for k in range(banks):
        source = lax.rem(bank - k + banks, banks)
        _, found = ranked_pairs(trig_ref, source * segs, segs, top, bank)
        for c in range(CAP):
            offset = off_ref[lax.rem(found[c], top), source * segs + found[c] // top]
            mult = jnp.where(line == k * CAP + c, 2 * offset + (LAGS - 1), mult)
    mult_ref[...] = mult
    for copy in copies:
        copy.wait()


def place_kernel(info_ref, trig_ref, *rest, banks, segs, top):
    back_refs = rest[:banks]
    out_ref, all_ref = rest[banks:]
    bank = info_ref[1]
    part = out_ref.shape[2]
    for k in range(banks):
        all_ref[CAP * k : CAP * (k + 1), :] = back_refs[k][...]
    for p in range(segs * top):
        target = trig_ref[p % top, bank * segs + p // top]
        rank = jnp.int32(0)
        for q in range(p):
            rank = rank + (trig_ref[q % top, bank * segs + q // top] == target).astype(jnp.int32)
        at = lax.rem(target - bank + banks, banks) * CAP + jnp.minimum(rank, CAP - 1)
        out_ref[p // top, p % top : p % top + 1, :] = all_ref[pl.ds(at, 1), :][:, :part]


def fine_kernel(info_ref, w_ref, mult_ref, g_ref, *rest, blocks, freqs, chunks, kc, period):
    slot_refs = rest[:blocks]
    keep_ref, send_ref = rest[blocks : blocks + 2]
    a_refs, b_refs, y_refs = (rest[blocks + i : blocks + i + 2] for i in (2, 4, 6))
    acc_ref, tab_ref, ctr_ref, held_ref, sems = rest[blocks + 8 :]
    base = info_ref[0]
    freq = info_ref[2]
    n = blocks * CAP
    cols = n * LAGS
    tsub = g_ref.shape[2]

    def fetch(chunk):
        at = pl.ds(pl.multiple_of(chunk * kc, kc), kc)
        return pltpu.make_async_copy(g_ref.at[:, 0, :, at], held_ref.at[chunk], sems.at[chunk])

    for chunk in range(chunks):
        fetch(chunk).start()

    def gen(which, chunk):
        a_ref, b_ref, y_ref = a_refs[which], b_refs[which], y_refs[which]
        shift = pl.multiple_of(chunk * kc, kc)
        w = w_ref[:, pl.ds(shift, kc)]
        for k in range(blocks):
            for i in range(CAP):
                x = slot_refs[k][i, :, pl.ds(shift, kc)].astype(F32) * w
                a_ref[0, CAP * k + i : CAP * k + i + 1, :] = x[0:1]
                a_ref[1, CAP * k + i : CAP * k + i + 1, :] = x[1:2]
        odd = 2 * lax.broadcasted_iota(jnp.int32, (PAIRS, LANES), 0) + 1
        dc, ds = sincos(shift * odd, period)
        ec, es = sincos(shift * mult_ref[...], period)
        for lo in range(0, kc, LANES):
            lanes = slice(lo, lo + LANES)
            c, s = rotate(ctr_ref[0, :, lanes], ctr_ref[1, :, lanes], ec, es)
            re = a_ref[0, :, lanes]
            im = a_ref[1, :, lanes]
            b_ref[0, :, lanes] = re * c - im * s
            b_ref[1, :, lanes] = re * s + im * c
            c, s = rotate(tab_ref[0, :, lanes], tab_ref[1, :, lanes], dc, ds)
            for i in range(n):
                re = b_ref[0, i : i + 1, lanes]
                im = b_ref[1, i : i + 1, lanes]
                rc = re * c
                js = im * s
                jc = im * c
                rs = re * s
                at = i * LAGS
                y_ref[at : at + LAGS, lanes] = jnp.concatenate([rc - js, rc + js], axis=0).astype(BF16)
                y_ref[cols + at : cols + at + LAGS, lanes] = jnp.concatenate(
                    [jc + rs, jc - rs], axis=0
                ).astype(BF16)

    ids = base + lax.broadcasted_iota(jnp.int32, (PAIRS, kc), 1)
    odd = 2 * lax.broadcasted_iota(jnp.int32, (PAIRS, kc), 0) + 1
    c, s = sincos(ids * odd, period)
    tab_ref[0] = c
    tab_ref[1] = s
    ids = base + lax.broadcasted_iota(jnp.int32, (n, kc), 1)
    c, s = sincos(ids * mult_ref[:, 0:1], period)
    ctr_ref[0] = c
    ctr_ref[1] = s
    acc_ref[...] = jnp.zeros_like(acc_ref)
    gen(0, jnp.int32(0))

    def pair(turn, carry):
        fetch(2 * turn).wait()
        fetch(2 * turn + 1).wait()
        for half in range(2):
            chunk = 2 * turn + half
            gen(1 - half, jnp.minimum(chunk + 1, chunks - 1))
            g = jnp.concatenate([held_ref[chunk, 0], held_ref[chunk, 1]], axis=0)
            acc_ref[...] += dot_t(y_refs[half][...], g)
        return carry

    lax.fori_loop(0, chunks // 2, pair, 0)
    part = tsub // freqs
    acc = acc_ref[...]
    swap = pltpu.roll(acc, LANES - tsub, 1)
    corr_real = acc[:cols] + swap[cols:]
    corr_imag = acc[cols:] - swap[:cols]
    lane = lax.broadcasted_iota(jnp.int32, (1, LANES), 1)

    def pack(dest):
        real, imag = corr_real, pltpu.roll(corr_imag, part, 1)
        for d in range(1, freqs):
            here = dest == d
            real = jnp.where(here, pltpu.roll(corr_real, LANES - d * part, 1), real)
            moved = corr_imag if d == 1 else pltpu.roll(corr_imag, LANES - (d - 1) * part, 1)
            imag = jnp.where(here, moved, imag)
        return jnp.where(lane < part, real, jnp.where(lane < 2 * part, imag, 0.0))

    keep_ref[...] = pack(freq)
    for k in range(1, freqs):
        send_ref[k - 1] = pack(lax.rem(freq + k, freqs))


def fine_final_kernel(keep_ref, norm_ref, *rest, freqs, n, part, line):
    recv_refs = rest[: 2 * (freqs - 1)]
    out_refs = rest[2 * (freqs - 1) :]
    x = keep_ref[...]
    norm = norm_ref[line : line + 1, :]
    for k in range(freqs - 1):
        x = x + recv_refs[2 * k][0]
        norm = norm + recv_refs[2 * k + 1][0, line : line + 1, :]
    e = x[: n * LAGS]
    e = e * e
    e = e + pltpu.roll(e, LANES - part, 1)
    for i in range(n):
        top = jnp.max(e[i * LAGS : (i + 1) * LAGS], axis=0, keepdims=True)
        out_refs[i // CAP][i % CAP : i % CAP + 1, :] = top / norm


def params(mib=50, **kw):
    return pltpu.CompilerParams(vmem_limit_bytes=mib * 1024 * 1024, **kw)


SMEM = pl.BlockSpec(memory_space=pltpu.SMEM)
VMEM = pl.BlockSpec(memory_space=pltpu.VMEM)
HBM = pl.BlockSpec(memory_space=pltpu.HBM)


def coarse_section(info, weight, templates, blocks, banks, freqs, period):
    segs = blocks[0].shape[0]
    rows, bins = templates.shape[1], templates.shape[2]
    total = banks * segs
    cols = total * LAGS
    kc = min(1024, bins // 2)
    chunks = bins // kc
    part = rows // freqs
    kernel = functools.partial(
        coarse_kernel, blocks=len(blocks), segs=segs, banks=banks, freqs=freqs, chunks=chunks, kc=kc, period=period
    )
    return pl.pallas_call(
        kernel,
        in_specs=[
            SMEM,
            VMEM,
            HBM,
        ]
        + [VMEM for _ in blocks],
        out_shape=[
            jax.ShapeDtypeStruct((part, 2 * cols), F32),
            jax.ShapeDtypeStruct((freqs - 1, part, 2 * cols), F32),
        ],
        scratch_shapes=[
            *[pltpu.VMEM((banks, 2 * segs, kc), F32) for _ in range(2)],
            *[pltpu.VMEM((4, total, kc), F32) for _ in range(2)],
            *[pltpu.VMEM((2 * cols, 2 * kc), BF16) for _ in range(2)],
            pltpu.VMEM((rows, 2 * cols), F32),
            pltpu.VMEM((2, PAIRS, kc), F32),
            pltpu.VMEM((2, PAIRS, kc), F32),
            pltpu.VMEM((chunks, 2, rows, kc), BF16),
            pltpu.SemaphoreType.DMA((chunks,)),
        ],
        compiler_params=params(),
        cost_estimate=pl.CostEstimate(
            flops=8 * rows * bins * cols, bytes_accessed=4 * rows * bins, transcendentals=0
        ),
        name="coarse",
    )(info, weight, templates, *blocks)


def fine_section(info, weight, mult, templates, blocks, freqs, period):
    bins = templates.shape[3]
    tsub = templates.shape[2]
    n = CAP * len(blocks)
    cols = n * LAGS
    kc = min(4096, bins // 2)
    chunks = bins // kc
    kernel = functools.partial(
        fine_kernel, blocks=len(blocks), freqs=freqs, chunks=chunks, kc=kc, period=period
    )
    return pl.pallas_call(
        kernel,
        in_specs=[
            SMEM,
            VMEM,
            VMEM,
            HBM,
        ]
        + [VMEM for _ in blocks],
        out_shape=[
            jax.ShapeDtypeStruct((cols, LANES), F32),
            jax.ShapeDtypeStruct((freqs - 1, cols, LANES), F32),
        ],
        scratch_shapes=[
            *[pltpu.VMEM((2, n, kc), F32) for _ in range(4)],
            *[pltpu.VMEM((2 * cols, kc), BF16) for _ in range(2)],
            pltpu.VMEM((2 * cols, LANES), F32),
            pltpu.VMEM((2, PAIRS, kc), F32),
            pltpu.VMEM((2, n, kc), F32),
            pltpu.VMEM((chunks, 2, tsub, kc), BF16),
            pltpu.SemaphoreType.DMA((chunks,)),
        ],
        compiler_params=params(),
        cost_estimate=pl.CostEstimate(
            flops=8 * tsub * bins * cols, bytes_accessed=4 * tsub * bins, transcendentals=0
        ),
        name="fine",
    )(info, weight, mult, templates, *blocks)


def after(value, *others):
    return lax.optimization_barrier((value, *others))[0]


def shift_permute(value, axis, count, by):
    return lax.ppermute(value, axis, [(i, (i + by) % count) for i in range(count)])


def norm_section(info, coarse_weight, fine_weight, coarse_templates, fine_templates, freqs):
    rows, bins = coarse_templates.shape[1:]
    tsub, fine_bins = fine_templates.shape[2:]
    chunks = 8
    lines = -(-(max(rows // freqs // LANES, 1) + 1) // 8) * 8
    return pl.pallas_call(
        functools.partial(norm_kernel, freqs=freqs),
        in_specs=[SMEM, VMEM, VMEM, HBM, HBM],
        out_shape=[
            jax.ShapeDtypeStruct((lines, LANES), F32),
            jax.ShapeDtypeStruct((freqs - 1, lines, LANES), F32),
        ],
        scratch_shapes=[
            pltpu.VMEM((rows, LANES), F32),
            pltpu.VMEM((tsub, LANES), F32),
            pltpu.VMEM((chunks, 2, rows, bins // chunks), BF16),
            pltpu.VMEM((chunks, 2, tsub, fine_bins // chunks), BF16),
            pltpu.SemaphoreType.DMA((chunks,)),
            pltpu.SemaphoreType.DMA((chunks,)),
        ],
        compiler_params=params(),
        cost_estimate=pl.CostEstimate(
            flops=10**9, bytes_accessed=4 * (rows * bins + tsub * fine_bins), transcendentals=0
        ),
        name="norms",
    )(info, coarse_weight, fine_weight, coarse_templates, fine_templates)


def body(
    coarse_spectra,
    fine_spectra,
    coarse_templates,
    fine_templates,
    coarse_weight,
    fine_weight,
    triggers,
    offsets,
):
    banks = lax.axis_size("bank")
    freqs = lax.axis_size("freq")
    bank = lax.axis_index("bank")
    freq = lax.axis_index("freq")
    segs = fine_spectra.shape[0]
    coarse_bins = coarse_spectra.shape[2]
    fine_bins = fine_spectra.shape[2]
    top = triggers.shape[1]
    tsub = fine_templates.shape[2]
    part = tsub // freqs
    coarse_period = 4 * coarse_bins * freqs
    fine_period = 4 * fine_bins * freqs
    zero = jnp.zeros((), jnp.int32)
    coarse_info = jnp.stack([freq * coarse_bins, bank, freq, zero]).astype(jnp.int32)
    fine_info = jnp.stack([freq * fine_bins, bank, freq, zero]).astype(jnp.int32)
    coarse_weight = coarse_weight.reshape(1, -1)
    fine_weight = fine_weight.reshape(1, -1)

    coarse_blocks = [coarse_spectra] + [
        shift_permute(coarse_spectra, "bank", banks, k) for k in range(1, banks)
    ]

    *picked, mult = pl.pallas_call(
        functools.partial(pick_kernel, banks=banks, segs=segs, top=top),
        in_specs=[SMEM, SMEM, SMEM, pl.BlockSpec(memory_space=pltpu.HBM)],
        out_shape=[jax.ShapeDtypeStruct((CAP, 2, fine_bins), BF16) for _ in range(banks)]
        + [jax.ShapeDtypeStruct((banks * CAP, LANES), jnp.int32)],
        scratch_shapes=[pltpu.SemaphoreType.DMA((banks * CAP,))],
        compiler_params=params(),
        name="pick",
    )(fine_info, triggers.T, offsets.T, fine_spectra)
    order = sorted(range(banks), key=lambda k: min(k, banks - k))
    fine_blocks = {}
    for place, k in enumerate(order):
        block = picked[k] if place < 2 else after(picked[k], *coarse_blocks)
        fine_blocks[k] = block if k == 0 else shift_permute(block, "bank", banks, k)

    line = max(coarse_templates.shape[1] // freqs // LANES, 1)

    def exchange(send):
        return [shift_permute(send[k - 1 : k], "freq", freqs, k) for k in range(1, freqs)]

    norms, send_norms = norm_section(
        after(coarse_info, mult), coarse_weight, fine_weight, coarse_templates, fine_templates, freqs
    )
    recv_norms = exchange(send_norms)
    keep, send = coarse_section(
        after(coarse_info, norms), coarse_weight, coarse_templates, coarse_blocks, banks, freqs, coarse_period
    )
    coarse_keep, coarse_received = keep, exchange(send)
    keep, send = fine_section(
        after(fine_info, coarse_keep),
        fine_weight,
        mult,
        fine_templates,
        [fine_blocks[k] for k in range(banks)],
        freqs,
        fine_period,
    )
    received = exchange(send)
    coarse_snr = pl.pallas_call(
        functools.partial(coarse_final_kernel, freqs=freqs, total=banks * segs),
        out_shape=jax.ShapeDtypeStruct((banks * segs, coarse_keep.shape[0]), F32),
        compiler_params=params(16),
        name="coarse_final",
    )(after(coarse_keep, keep), norms, *[x for pair in zip(coarse_received, recv_norms) for x in pair])
    results = pl.pallas_call(
        functools.partial(fine_final_kernel, freqs=freqs, n=CAP * banks, part=part, line=line),
        out_shape=[jax.ShapeDtypeStruct((CAP, LANES), F32) for _ in range(banks)],
        compiler_params=params(8),
        name="fine_final",
    )(after(keep, coarse_snr), norms, *[x for pair in zip(received, recv_norms) for x in pair])
    back = [
        results[k] if k == 0 else shift_permute(results[k], "bank", banks, banks - k)
        for k in range(banks)
    ]
    fine_snr = pl.pallas_call(
        functools.partial(place_kernel, banks=banks, segs=segs, top=top),
        in_specs=[SMEM, SMEM] + [pl.BlockSpec(memory_space=pltpu.VMEM) for _ in range(banks)],
        out_shape=jax.ShapeDtypeStruct((segs, top, part), F32),
        scratch_shapes=[pltpu.VMEM((banks * CAP, LANES), F32)],
        compiler_params=params(8),
        name="place",
    )(fine_info, triggers.T, *back)
    return (coarse_snr.T, fine_snr)


def solution(mesh):
    return sharded(mesh)


def sharded(mesh):
    return jax.shard_map(
        body,
        mesh=mesh,
        in_specs=(
            P(("groups", "seg", "bank"), None, "freq"),
            P(("groups", "seg", "bank"), None, "freq"),
            P(None, "bank", "freq"),
            P(None, "bank", None, "freq"),
            P(("groups", "freq")),
            P(("groups", "freq")),
            P(("groups", "seg"), None),
            P(("groups", "seg"), None),
        ),
        out_specs=(
            P(("bank", "freq"), ("groups", "seg")),
            P(("groups", "seg", "bank"), None, "freq"),
        ),
        check_vma=False,
    )
```

```python
import functools
import math

import jax
import jax.numpy as jnp
from jax import lax
from jax.experimental import pallas as pl
from jax.experimental.pallas import tpu as pltpu
from jax.sharding import PartitionSpec as P


CAP = 2
LAGS = 16
PAIRS = LAGS // 2
CSTRIDE = 2047
LANES = 128
F32 = jnp.float32
BF16 = jnp.bfloat16


def sincos(counts, period):
    half = period // 2
    signed = ((counts + half) & (period - 1)) - half
    x = signed.astype(F32) * (1.0 / period)
    u = x * x
    p = math.pi
    s = -(p**11) / 39916800.0
    for a in (p**9 / 362880.0, -(p**7) / 5040.0, p**5 / 120.0, -(p**3) / 6.0, p):
        s = s * u + a
    s = s * x
    c = p**12 / 479001600.0
    for a in (-(p**10) / 3628800.0, p**8 / 40320.0, -(p**6) / 720.0, p**4 / 24.0, -(p**2) / 2.0, 1.0):
        c = c * u + a
    return 1.0 - 2.0 * s * s, 2.0 * s * c


def dot_t(a, b):
    return lax.dot_general(a, b, (((1,), (1,)), ((), ())), preferred_element_type=F32)


def rotate(c, s, dc, ds):
    return c * dc - s * ds, s * dc + c * ds


def norm_add(acc_ref, w_ref, held_ref, chunk, turn, turns):
    rows = acc_ref.shape[0]
    bins = held_ref.shape[3]
    count = max(rows // turns, 16)
    r = turn * count
    if r >= rows:
        return
    n = acc_ref[r : r + count, :]
    for lo in range(0, bins, LANES):
        re = held_ref[chunk, 0, r : r + count, lo : lo + LANES].astype(F32)
        im = held_ref[chunk, 1, r : r + count, lo : lo + LANES].astype(F32)
        w = w_ref[:, pl.ds(pl.multiple_of(chunk * bins + lo, LANES), LANES)]
        n = n + (re * re + im * im) * w
    acc_ref[r : r + count, :] = n


def norm_row(n):
    if n.shape[0] < LANES:
        n = jnp.concatenate([n, jnp.zeros((LANES - n.shape[0], LANES), F32)], axis=0)
    return jnp.sum(n.T, axis=0, keepdims=True)


def coarse_kernel(
    info_ref, w_ref, h_ref, *rest, blocks, segs, banks, freqs, chunks, kc, period
):
    spec_refs = rest[:blocks]
    keep_ref, send_ref = rest[blocks : blocks + 2]
    a_refs, b_refs, y_refs = (rest[blocks + i : blocks + i + 2] for i in (2, 4, 6))
    acc_ref, tab_ref, ctr_ref, held_ref, sems = rest[blocks + 8 :]
    base = info_ref[0]
    bank = info_ref[1]
    freq = info_ref[2]
    total = banks * segs
    cols = total * LAGS

    def fetch(chunk):
        at = pl.ds(pl.multiple_of(chunk * kc, kc), kc)
        return pltpu.make_async_copy(h_ref.at[:, :, at], held_ref.at[chunk], sems.at[chunk])

    for chunk in range(chunks):
        fetch(chunk).start()

    def gen(which, chunk):
        a_ref, b_ref, y_ref = a_refs[which], b_refs[which], y_refs[which]
        shift = pl.multiple_of(chunk * kc, kc)
        w = w_ref[:, pl.ds(shift, kc)]
        for k in range(blocks):
            source = lax.rem(bank - k + banks, banks)
            for i in range(segs):
                a_ref[source, 2 * i : 2 * i + 2, :] = spec_refs[k][i, :, pl.ds(shift, kc)].astype(F32) * w
        odd = 2 * lax.broadcasted_iota(jnp.int32, (PAIRS, LANES), 0) + 1
        dc, ds = sincos(shift * odd * CSTRIDE, period)
        ec, es = sincos(jnp.full((PAIRS, LANES), shift * (15 * CSTRIDE), jnp.int32), period)
        for lo in range(0, kc, LANES):
            lanes = slice(lo, lo + LANES)
            c, s = rotate(ctr_ref[0, :, lanes], ctr_ref[1, :, lanes], ec, es)
            for b in range(0, total, 4):
                re, im = (
                    jnp.concatenate(
                        [a_ref[(b + i) // segs, 2 * ((b + i) % segs) + c : 2 * ((b + i) % segs) + c + 1, lanes] for i in range(4)],
                        axis=0,
                    )
                    for c in range(2)
                )
                b_ref[0, b : b + 4, lanes] = re * c[:4] - im * s[:4]
                b_ref[1, b : b + 4, lanes] = re * s[:4] + im * c[:4]
            c, s = rotate(tab_ref[0, :, lanes], tab_ref[1, :, lanes], dc, ds)
            b_ref[2, :PAIRS, lanes] = c
            b_ref[3, :PAIRS, lanes] = s
            re = b_ref[0, :, lanes]
            im = b_ref[1, :, lanes]
            for m in range(PAIRS):
                cm = b_ref[2, m : m + 1, lanes]
                sm = b_ref[3, m : m + 1, lanes]
                rc = re * cm
                js = im * sm
                jc = im * cm
                rs = re * sm
                for sign, (yr, yi) in enumerate(((rc - js, jc + rs), (rc + js, jc - rs))):
                    at = (2 * m + sign) * total
                    yr = yr.astype(BF16)
                    yi = yi.astype(BF16)
                    y_ref[at : at + total, lo : lo + LANES] = yr
                    y_ref[at : at + total, kc + lo : kc + lo + LANES] = yi
                    y_ref[cols + at : cols + at + total, lo : lo + LANES] = yi
                    y_ref[cols + at : cols + at + total, kc + lo : kc + lo + LANES] = -yr

    ids = base + lax.broadcasted_iota(jnp.int32, (PAIRS, kc), 1)
    odd = 2 * lax.broadcasted_iota(jnp.int32, (PAIRS, kc), 0) + 1
    c, s = sincos(ids * odd * CSTRIDE, period)
    tab_ref[0] = c
    tab_ref[1] = s
    c, s = sincos(ids * (15 * CSTRIDE), period)
    ctr_ref[0] = c
    ctr_ref[1] = s
    acc_ref[...] = jnp.zeros_like(acc_ref)
    gen(0, jnp.int32(0))

    def pair(turn, carry):
        fetch(2 * turn).wait()
        fetch(2 * turn + 1).wait()
        for half in range(2):
            chunk = 2 * turn + half
            gen(1 - half, jnp.minimum(chunk + 1, chunks - 1))
            h = jnp.concatenate([held_ref[chunk, 0], held_ref[chunk, 1]], axis=1)
            acc_ref[...] += dot_t(h, y_refs[half][...])
        return carry

    lax.fori_loop(0, chunks // 2, pair, 0)
    part = acc_ref.shape[0] // freqs
    keep_ref[...] = acc_ref[pl.ds(pl.multiple_of(freq * part, part), part), :]
    for k in range(1, freqs):
        dest = pl.multiple_of(lax.rem(freq + k, freqs) * part, part)
        send_ref[k - 1] = acc_ref[pl.ds(dest, part), :]


def norm_kernel(
    info_ref, cw_ref, fw_ref, h_ref, g_ref, keep_ref, send_ref, c_ref, f_ref, h_held, g_held, h_sems, g_sems, *, freqs
):
    chunks, _, rows, kc = h_held.shape
    tsub, kf = g_held.shape[2:]

    def fetch(i):
        at = pl.ds(pl.multiple_of(i * kc, kc), kc)
        yield pltpu.make_async_copy(h_ref.at[:, :, at], h_held.at[i], h_sems.at[i])
        at = pl.ds(pl.multiple_of(i * kf, kf), kf)
        yield pltpu.make_async_copy(g_ref.at[:, 0, :, at], g_held.at[i], g_sems.at[i])

    for i in range(chunks):
        for copy in fetch(i):
            copy.start()
    c_ref[...] = jnp.zeros_like(c_ref)
    f_ref[...] = jnp.zeros_like(f_ref)

    def turn(i, carry):
        for copy in fetch(i):
            copy.wait()
        for t in range(8):
            norm_add(c_ref, cw_ref, h_held, i, t, 8)
        for t in range(4):
            norm_add(f_ref, fw_ref, g_held, i, t, 4)
        return carry

    lax.fori_loop(0, chunks, turn, 0)
    part = rows // freqs
    fine_part = tsub // freqs
    size = min(part, LANES)

    def lay(ref, dest):
        ref[...] = jnp.zeros_like(ref)
        for r in range(0, part, size):
            row = norm_row(c_ref[pl.ds(pl.multiple_of(dest * part + r, size), size), :])
            ref[r // size : r // size + 1, :] = row
        row = norm_row(f_ref[pl.ds(pl.multiple_of(dest * fine_part, fine_part), fine_part), :])
        ref[part // size : part // size + 1, :] = row

    lay(keep_ref, info_ref[2])
    for k in range(1, freqs):
        lay(send_ref.at[k - 1], lax.rem(info_ref[2] + k, freqs))


def coarse_final_kernel(keep_ref, norm_ref, *rest, freqs, total):
    recv_refs = rest[: 2 * (freqs - 1)]
    out_ref = rest[2 * (freqs - 1)]
    part = keep_ref.shape[0]
    cols = total * LAGS
    corr = keep_ref[...]
    norms = norm_ref[...]
    for k in range(freqs - 1):
        corr = corr + recv_refs[2 * k][0]
        norms = norms + recv_refs[2 * k + 1][0]
    cr = corr[:part, :cols]
    ci = corr[:part, cols:]
    e = cr * cr + ci * ci
    width = cols
    while width > max(total, LANES):
        width //= 2
        e = jnp.maximum(e[:, :width], e[:, width:])
    while width > total:
        width //= 2
        e = jnp.maximum(e, pltpu.roll(e, LANES - width, 1))
    size = min(part, LANES)
    for r in range(0, part, size):
        rows = e[r : r + size]
        if size < LANES:
            rows = jnp.concatenate([rows, jnp.zeros((LANES - size, LANES), F32)], axis=0)
        out = rows.T[:total] / norms[r // size : r // size + 1]
        out_ref[:, r : r + size] = out[:, :size]


def ranked_pairs(trig_ref, first, segs, top, target):
    taken = jnp.int32(0)
    found = [jnp.int32(0) for _ in range(CAP)]
    for p in range(segs * top):
        hit = (trig_ref[p % top, first + p // top] == target).astype(jnp.int32)
        for c in range(CAP):
            found[c] = jnp.where(jnp.logical_and(hit == 1, taken == c), p, found[c])
        taken = taken + hit
    return taken, found


def pick_kernel(info_ref, trig_ref, spec_ref, *rest, banks, segs, top):
    out_refs = rest[:banks]
    mult_ref, sems = rest[banks:]
    bank = info_ref[1]
    copies = []
    for k in range(banks):
        k = (k + 1) % banks
        dest = lax.rem(bank + k, banks)
        _, found = ranked_pairs(trig_ref, bank * segs, segs, top, dest)
        for c in range(CAP):
            copy = pltpu.make_async_copy(
                spec_ref.at[found[c] // top], out_refs[k].at[c], sems.at[k * CAP + c]
            )
            copy.start()
            copies.append(copy)
    line = lax.broadcasted_iota(jnp.int32, mult_ref.shape, 0)
    mult = jnp.zeros(mult_ref.shape, jnp.int32)
    for k in range(banks):
        source = lax.rem(bank - k + banks, banks)
        _, found = ranked_pairs(trig_ref, source * segs, segs, top, bank)
        for c in range(CAP):
            offset = trig_ref[top + lax.rem(found[c], top), source * segs + found[c] // top]
            mult = jnp.where(line == k * CAP + c, 2 * offset + (LAGS - 1), mult)
    mult_ref[...] = mult
    for copy in copies:
        copy.wait()


def place_kernel(info_ref, trig_ref, *rest, banks, segs, top):
    back_refs = rest[:banks]
    out_ref, all_ref = rest[banks:]
    bank = info_ref[1]
    part = out_ref.shape[2]
    for k in range(banks):
        all_ref[CAP * k : CAP * (k + 1), :] = back_refs[k][...]
    for p in range(segs * top):
        target = trig_ref[p % top, bank * segs + p // top]
        rank = jnp.int32(0)
        for q in range(p):
            rank = rank + (trig_ref[q % top, bank * segs + q // top] == target).astype(jnp.int32)
        at = lax.rem(target - bank + banks, banks) * CAP + jnp.minimum(rank, CAP - 1)
        out_ref[p // top, p % top : p % top + 1, :] = all_ref[pl.ds(at, 1), :][:, :part]


def fine_kernel(info_ref, w_ref, mult_ref, g_ref, *rest, blocks, freqs, chunks, kc, period):
    slot_refs = rest[:blocks]
    keep_ref, send_ref = rest[blocks : blocks + 2]
    a_refs, b_refs, y_refs = (rest[blocks + i : blocks + i + 2] for i in (2, 4, 6))
    acc_ref, tab_ref, ctr_ref, held_ref, sems = rest[blocks + 8 :]
    base = info_ref[0]
    freq = info_ref[2]
    n = blocks * CAP
    cols = n * LAGS
    tsub = g_ref.shape[2]

    def fetch(chunk):
        at = pl.ds(pl.multiple_of(chunk * kc, kc), kc)
        return pltpu.make_async_copy(g_ref.at[:, 0, :, at], held_ref.at[chunk], sems.at[chunk])

    for chunk in range(chunks):
        fetch(chunk).start()

    def gen(which, chunk):
        a_ref, b_ref, y_ref = a_refs[which], b_refs[which], y_refs[which]
        shift = pl.multiple_of(chunk * kc, kc)
        w = w_ref[:, pl.ds(shift, kc)]
        for k in range(blocks):
            for i in range(CAP):
                x = slot_refs[k][i, :, pl.ds(shift, kc)].astype(F32) * w
                a_ref[0, CAP * k + i : CAP * k + i + 1, :] = x[0:1]
                a_ref[1, CAP * k + i : CAP * k + i + 1, :] = x[1:2]
        odd = 2 * lax.broadcasted_iota(jnp.int32, (PAIRS, LANES), 0) + 1
        dc, ds = sincos(shift * odd, period)
        ec, es = sincos(shift * mult_ref[...], period)
        for lo in range(0, kc, LANES):
            lanes = slice(lo, lo + LANES)
            c, s = rotate(ctr_ref[0, :, lanes], ctr_ref[1, :, lanes], ec, es)
            re = a_ref[0, :, lanes]
            im = a_ref[1, :, lanes]
            b_ref[0, :, lanes] = re * c - im * s
            b_ref[1, :, lanes] = re * s + im * c
            c, s = rotate(tab_ref[0, :, lanes], tab_ref[1, :, lanes], dc, ds)
            for i in range(n):
                re = b_ref[0, i : i + 1, lanes]
                im = b_ref[1, i : i + 1, lanes]
                rc = re * c
                js = im * s
                jc = im * c
                rs = re * s
                at = i * LAGS
                y_ref[at : at + LAGS, lanes] = jnp.concatenate([rc - js, rc + js], axis=0).astype(BF16)
                y_ref[cols + at : cols + at + LAGS, lanes] = jnp.concatenate(
                    [jc + rs, jc - rs], axis=0
                ).astype(BF16)

    ids = base + lax.broadcasted_iota(jnp.int32, (PAIRS, kc), 1)
    odd = 2 * lax.broadcasted_iota(jnp.int32, (PAIRS, kc), 0) + 1
    c, s = sincos(ids * odd, period)
    tab_ref[0] = c
    tab_ref[1] = s
    ids = base + lax.broadcasted_iota(jnp.int32, (n, kc), 1)
    c, s = sincos(ids * mult_ref[:, 0:1], period)
    ctr_ref[0] = c
    ctr_ref[1] = s
    acc_ref[...] = jnp.zeros_like(acc_ref)
    gen(0, jnp.int32(0))

    def pair(turn, carry):
        fetch(2 * turn).wait()
        fetch(2 * turn + 1).wait()
        for half in range(2):
            chunk = 2 * turn + half
            gen(1 - half, jnp.minimum(chunk + 1, chunks - 1))
            g = jnp.concatenate([held_ref[chunk, 0], held_ref[chunk, 1]], axis=0)
            acc_ref[...] += dot_t(y_refs[half][...], g)
        return carry

    lax.fori_loop(0, chunks // 2, pair, 0)
    part = tsub // freqs
    acc = acc_ref[...]
    swap = pltpu.roll(acc, LANES - tsub, 1)
    corr_real = acc[:cols] + swap[cols:]
    corr_imag = acc[cols:] - swap[:cols]
    lane = lax.broadcasted_iota(jnp.int32, (1, LANES), 1)

    def pack(dest):
        real, imag = corr_real, pltpu.roll(corr_imag, part, 1)
        for d in range(1, freqs):
            here = dest == d
            real = jnp.where(here, pltpu.roll(corr_real, LANES - d * part, 1), real)
            moved = corr_imag if d == 1 else pltpu.roll(corr_imag, LANES - (d - 1) * part, 1)
            imag = jnp.where(here, moved, imag)
        return jnp.where(lane < part, real, jnp.where(lane < 2 * part, imag, 0.0))

    keep_ref[...] = pack(freq)
    for k in range(1, freqs):
        send_ref[k - 1] = pack(lax.rem(freq + k, freqs))


def fine_final_kernel(keep_ref, norm_ref, *rest, freqs, n, part, line):
    recv_refs = rest[: 2 * (freqs - 1)]
    out_refs = rest[2 * (freqs - 1) :]
    x = keep_ref[...]
    norm = norm_ref[line : line + 1, :]
    for k in range(freqs - 1):
        x = x + recv_refs[2 * k][0]
        norm = norm + recv_refs[2 * k + 1][0, line : line + 1, :]
    e = x[: n * LAGS]
    e = e * e
    e = e + pltpu.roll(e, LANES - part, 1)
    for i in range(n):
        top = jnp.max(e[i * LAGS : (i + 1) * LAGS], axis=0, keepdims=True)
        out_refs[i // CAP][i % CAP : i % CAP + 1, :] = top / norm


def params(mib=50, **kw):
    return pltpu.CompilerParams(vmem_limit_bytes=mib * 1024 * 1024, **kw)


SMEM = pl.BlockSpec(memory_space=pltpu.SMEM)
VMEM = pl.BlockSpec(memory_space=pltpu.VMEM)
HBM = pl.BlockSpec(memory_space=pltpu.HBM)


def coarse_section(info, weight, templates, blocks, banks, freqs, period):
    segs = blocks[0].shape[0]
    rows, bins = templates.shape[1], templates.shape[2]
    total = banks * segs
    cols = total * LAGS
    kc = min(1024, bins // 2)
    chunks = bins // kc
    part = rows // freqs
    kernel = functools.partial(
        coarse_kernel, blocks=len(blocks), segs=segs, banks=banks, freqs=freqs, chunks=chunks, kc=kc, period=period
    )
    return pl.pallas_call(
        kernel,
        in_specs=[
            SMEM,
            VMEM,
            HBM,
        ]
        + [VMEM for _ in blocks],
        out_shape=[
            jax.ShapeDtypeStruct((part, 2 * cols), F32),
            jax.ShapeDtypeStruct((freqs - 1, part, 2 * cols), F32),
        ],
        scratch_shapes=[
            *[pltpu.VMEM((banks, 2 * segs, kc), F32) for _ in range(2)],
            *[pltpu.VMEM((4, total, kc), F32) for _ in range(2)],
            *[pltpu.VMEM((2 * cols, 2 * kc), BF16) for _ in range(2)],
            pltpu.VMEM((rows, 2 * cols), F32),
            pltpu.VMEM((2, PAIRS, kc), F32),
            pltpu.VMEM((2, PAIRS, kc), F32),
            pltpu.VMEM((chunks, 2, rows, kc), BF16),
            pltpu.SemaphoreType.DMA((chunks,)),
        ],
        compiler_params=params(),
        cost_estimate=pl.CostEstimate(
            flops=8 * rows * bins * cols, bytes_accessed=4 * rows * bins, transcendentals=0
        ),
        name="coarse",
    )(info, weight, templates, *blocks)


def fine_section(info, weight, mult, templates, blocks, freqs, period):
    bins = templates.shape[3]
    tsub = templates.shape[2]
    n = CAP * len(blocks)
    cols = n * LAGS
    kc = min(4096, bins // 2)
    chunks = bins // kc
    kernel = functools.partial(
        fine_kernel, blocks=len(blocks), freqs=freqs, chunks=chunks, kc=kc, period=period
    )
    return pl.pallas_call(
        kernel,
        in_specs=[
            SMEM,
            VMEM,
            VMEM,
            HBM,
        ]
        + [VMEM for _ in blocks],
        out_shape=[
            jax.ShapeDtypeStruct((cols, LANES), F32),
            jax.ShapeDtypeStruct((freqs - 1, cols, LANES), F32),
        ],
        scratch_shapes=[
            *[pltpu.VMEM((2, n, kc), F32) for _ in range(4)],
            *[pltpu.VMEM((2 * cols, kc), BF16) for _ in range(2)],
            pltpu.VMEM((2 * cols, LANES), F32),
            pltpu.VMEM((2, PAIRS, kc), F32),
            pltpu.VMEM((2, n, kc), F32),
            pltpu.VMEM((chunks, 2, tsub, kc), BF16),
            pltpu.SemaphoreType.DMA((chunks,)),
        ],
        compiler_params=params(),
        cost_estimate=pl.CostEstimate(
            flops=8 * tsub * bins * cols, bytes_accessed=4 * tsub * bins, transcendentals=0
        ),
        name="fine",
    )(info, weight, mult, templates, *blocks)


def after(value, *others):
    return lax.optimization_barrier((value, *others))[0]


def shift_permute(value, axis, count, by):
    return lax.ppermute(value, axis, [(i, (i + by) % count) for i in range(count)])


def norm_section(info, coarse_weight, fine_weight, coarse_templates, fine_templates, freqs):
    rows, bins = coarse_templates.shape[1:]
    tsub, fine_bins = fine_templates.shape[2:]
    chunks = 8
    lines = -(-(max(rows // freqs // LANES, 1) + 1) // 8) * 8
    return pl.pallas_call(
        functools.partial(norm_kernel, freqs=freqs),
        in_specs=[SMEM, VMEM, VMEM, HBM, HBM],
        out_shape=[
            jax.ShapeDtypeStruct((lines, LANES), F32),
            jax.ShapeDtypeStruct((freqs - 1, lines, LANES), F32),
        ],
        scratch_shapes=[
            pltpu.VMEM((rows, LANES), F32),
            pltpu.VMEM((tsub, LANES), F32),
            pltpu.VMEM((chunks, 2, rows, bins // chunks), BF16),
            pltpu.VMEM((chunks, 2, tsub, fine_bins // chunks), BF16),
            pltpu.SemaphoreType.DMA((chunks,)),
            pltpu.SemaphoreType.DMA((chunks,)),
        ],
        compiler_params=params(),
        cost_estimate=pl.CostEstimate(
            flops=10**9, bytes_accessed=4 * (rows * bins + tsub * fine_bins), transcendentals=0
        ),
        name="norms",
    )(info, coarse_weight, fine_weight, coarse_templates, fine_templates)


def body(
    coarse_spectra,
    fine_spectra,
    coarse_templates,
    fine_templates,
    coarse_weight,
    fine_weight,
    triggers,
    offsets,
):
    banks = lax.axis_size("bank")
    freqs = lax.axis_size("freq")
    bank = lax.axis_index("bank")
    freq = lax.axis_index("freq")
    segs = fine_spectra.shape[0]
    coarse_bins = coarse_spectra.shape[2]
    fine_bins = fine_spectra.shape[2]
    top = triggers.shape[1]
    tsub = fine_templates.shape[2]
    part = tsub // freqs
    coarse_period = 4 * coarse_bins * freqs
    fine_period = 4 * fine_bins * freqs
    zero = jnp.zeros((), jnp.int32)
    coarse_info = jnp.stack([freq * coarse_bins, bank, freq, zero]).astype(jnp.int32)
    fine_info = jnp.stack([freq * fine_bins, bank, freq, zero]).astype(jnp.int32)
    coarse_weight = coarse_weight.reshape(1, -1)
    fine_weight = fine_weight.reshape(1, -1)

    coarse_blocks = [coarse_spectra] + [
        shift_permute(coarse_spectra, "bank", banks, k) for k in range(1, banks)
    ]

    named = jnp.concatenate([triggers.T, offsets.T], axis=0)
    *picked, mult = pl.pallas_call(
        functools.partial(pick_kernel, banks=banks, segs=segs, top=top),
        in_specs=[SMEM, SMEM, HBM],
        out_shape=[jax.ShapeDtypeStruct((CAP, 2, fine_bins), BF16) for _ in range(banks)]
        + [jax.ShapeDtypeStruct((banks * CAP, LANES), jnp.int32)],
        scratch_shapes=[pltpu.SemaphoreType.DMA((banks * CAP,))],
        compiler_params=params(),
        name="pick",
    )(fine_info, named, fine_spectra)
    order = sorted(range(banks), key=lambda k: min(k, banks - k))
    fine_blocks = {}
    for k in order:
        fine_blocks[k] = picked[k] if k == 0 else shift_permute(picked[k], "bank", banks, k)

    line = max(coarse_templates.shape[1] // freqs // LANES, 1)

    def exchange(send):
        return [shift_permute(send[k - 1 : k], "freq", freqs, k) for k in range(1, freqs)]

    norms, send_norms = norm_section(
        after(coarse_info, mult), coarse_weight, fine_weight, coarse_templates, fine_templates, freqs
    )
    recv_norms = exchange(send_norms)
    keep, send = coarse_section(
        after(coarse_info, norms), coarse_weight, coarse_templates, coarse_blocks, banks, freqs, coarse_period
    )
    coarse_keep, coarse_received = keep, exchange(send)
    keep, send = fine_section(
        after(fine_info, coarse_keep),
        fine_weight,
        mult,
        fine_templates,
        [fine_blocks[k] for k in range(banks)],
        freqs,
        fine_period,
    )
    received = exchange(send)
    coarse_snr = pl.pallas_call(
        functools.partial(coarse_final_kernel, freqs=freqs, total=banks * segs),
        out_shape=jax.ShapeDtypeStruct((banks * segs, coarse_keep.shape[0]), F32),
        compiler_params=params(16),
        name="coarse_final",
    )(after(coarse_keep, keep), norms, *[x for pair in zip(coarse_received, recv_norms) for x in pair])
    results = pl.pallas_call(
        functools.partial(fine_final_kernel, freqs=freqs, n=CAP * banks, part=part, line=line),
        out_shape=[jax.ShapeDtypeStruct((CAP, LANES), F32) for _ in range(banks)],
        compiler_params=params(8),
        name="fine_final",
    )(after(keep, coarse_snr), norms, *[x for pair in zip(received, recv_norms) for x in pair])
    back = [
        results[k] if k == 0 else shift_permute(results[k], "bank", banks, banks - k)
        for k in range(banks)
    ]
    fine_snr = pl.pallas_call(
        functools.partial(place_kernel, banks=banks, segs=segs, top=top),
        in_specs=[SMEM, SMEM] + [pl.BlockSpec(memory_space=pltpu.VMEM) for _ in range(banks)],
        out_shape=jax.ShapeDtypeStruct((segs, top, part), F32),
        scratch_shapes=[pltpu.VMEM((banks * CAP, LANES), F32)],
        compiler_params=params(8),
        name="place",
    )(fine_info, named, *back)
    return (coarse_snr.T, fine_snr)


def solution(mesh):
    return sharded(mesh)


def sharded(mesh):
    return jax.shard_map(
        body,
        mesh=mesh,
        in_specs=(
            P(("groups", "seg", "bank"), None, "freq"),
            P(("groups", "seg", "bank"), None, "freq"),
            P(None, "bank", "freq"),
            P(None, "bank", None, "freq"),
            P(("groups", "freq")),
            P(("groups", "freq")),
            P(("groups", "seg"), None),
            P(("groups", "seg"), None),
        ),
        out_specs=(
            P(("bank", "freq"), ("groups", "seg")),
            P(("groups", "seg", "bank"), None, "freq"),
        ),
        check_vma=False,
    )
```
